256 devices in a mesh: member: 16 (over z_hi, y), lat: 4 (over z_lo, core), lon: 4 (over x).
Axes of the slice: x: 4, y: 4, z: 8 (z_hi: 4, z_lo: 2; z = z_hi * 2 + z_lo), core: 2. Of those that a mesh axis runs over, the one named last changes fastest.
Arguments:
- layer_inputs: bfloat16 [16, 256, 192, 512], P('member', None, 'lat', 'lon'), may hold values from -6 to 6
- conv_weight: bfloat16 [3, 3, 69, 256], replicated, may hold values from -0.125 to 0.125
- channel_offset: float32 [69], replicated, may hold values from -4 to 4
- observed: bfloat16 [69, 192, 512], P(None, 'lat', 'lon'), may hold values from -6 to 6
- var_weight: float32 [69], replicated, may hold values from 0.5 to 4
Outputs:
- predicted_fields: bfloat16 [16, 69, 192, 512], P('member', None, 'lat', 'lon')
- input_slope_field: bfloat16 [16, 256, 192, 512], P('member', None, 'lat', 'lon')
The draws below stay inside these ranges and needn't reach their ends.
All inputs are finite; a program needn't handle non-finite values.
Results may differ from the reference program's by a relative error of at most 0.0063.
Values may be sent and summed in bfloat16 or wider, within the bound.
A program may use at most 192 MiB of HBM per device.

```python
import math
import jax
import jax.numpy as jnp
from jax import lax

C = 256
OV = 69
MEMBERS = 16
NLAT = 192
NLON = 512


def steps_of(key, dims, cuts, low, top_value):
    def one(axis_at, shards_of):
        heights = jax.random.uniform(jax.random.fold_in(jax.random.fold_in(key, 6), axis_at), (shards_of,), jnp.float32, low / len(cuts), top_value / len(cuts))
        return jnp.repeat(jnp.exp(heights), dims[axis_at] // shards_of).reshape((-1,) + (1,) * (len(dims) - axis_at - 1))

    loudness = one(*cuts[0])
    for cut in cuts[1:]:
        loudness = loudness * one(*cut)
    return loudness


def gaussian(rng, extent, scale, bound, shards=(), kind=jnp.bfloat16):
    array = jax.random.normal(rng, extent, jnp.float32) * scale
    if len(shards) > 0:
        array = steps_of(rng, extent, shards, -0.22, 0.18) * array
    return jnp.clip(array, min=-bound, max=bound).astype(kind)


def setup_inputs(seed: int = 0) -> dict:
    streams_of = jax.random.split(jax.random.key(seed), 6)
    layer_inputs = gaussian(streams_of[0], (MEMBERS, C, NLAT, NLON), 1.0, 6.0, ((0, 16), (2, 4), (3, 4)))
    conv_weight = gaussian(streams_of[1], (3, 3, OV, C), (9 * C) ** -0.5, 0.125)
    channel_offset = gaussian(streams_of[2], (OV,), 1.0, 4.0, (), jnp.float32)
    observed = gaussian(streams_of[3], (OV, NLAT, NLON), 1.0, 6.0, ((1, 4), (2, 4)))
    var_weight = jnp.clip(jnp.exp(jax.random.uniform(streams_of[4], (OV,), jnp.float32, math.log(0.5), math.log(4.0))), 0.5, 4.0)
    return {"layer_inputs": layer_inputs, "conv_weight": conv_weight, "channel_offset": channel_offset, "observed": observed, "var_weight": var_weight}


smoothing = 0.25

def smooth(difference):
    return difference * lax.rsqrt(difference * difference + smoothing * smoothing)

def cycle_pad(field):
    widened = jnp.concatenate([field[..., -1:], field, field[..., :1]], axis=-1)
    zeros = jnp.zeros_like(widened[..., :1, :])
    return jnp.concatenate([zeros, widened, zeros], axis=-2)

def reference(layer_inputs, conv_weight, channel_offset, observed, var_weight):

    def apply_output_layer(member_features):
        padded = cycle_pad(member_features)
        accumulated_outcome = jnp.zeros((OV, NLAT * NLON), jnp.float32)
        for row_tap in range(3):
            for col_tap in range(3):
                window = padded[:, row_tap:row_tap + NLAT, col_tap:col_tap + NLON].reshape(C, NLAT * NLON)
                accumulated_outcome = accumulated_outcome + jnp.dot(conv_weight[row_tap, col_tap], window, preferred_element_type=jnp.float32)
        return (accumulated_outcome.reshape(OV, NLAT, NLON) + channel_offset[:, None, None]).astype(jnp.bfloat16)
    predicted_fields = lax.map(apply_output_layer, layer_inputs)
    quantity_table = predicted_fields.astype(jnp.float32)

    def add_member(running, member_values):
        return (running + smooth(quantity_table - member_values[None]), None)
    pair_sums, unused = lax.scan(add_member, jnp.zeros_like(quantity_table), quantity_table)
    row_index = jnp.arange(NLAT).astype(jnp.float32)
    lat_weight = jnp.cos((-80.0 + 160.0 * (row_index + 0.5) / NLAT) * (jnp.pi / 180.0))
    target = observed.astype(jnp.float32)[None]
    gradient = (lat_weight[:, None] * var_weight[:, None, None] * (smooth(quantity_table - target) - pair_sums / (MEMBERS - 1))).astype(jnp.bfloat16)

    def backward(member_gradient):
        padded = cycle_pad(member_gradient)
        accumulated_outcome = jnp.zeros((C, NLAT * NLON), jnp.float32)
        for row_tap in range(3):
            for col_tap in range(3):
                window = padded[:, 2 - row_tap:2 - row_tap + NLAT, 2 - col_tap:2 - col_tap + NLON].reshape(OV, NLAT * NLON)
                accumulated_outcome = accumulated_outcome + jnp.dot(conv_weight[row_tap, col_tap].T, window, preferred_element_type=jnp.float32)
        return accumulated_outcome.reshape(C, NLAT, NLON).astype(jnp.bfloat16)
    input_slope_field = lax.map(backward, gradient)
    return (predicted_fields, input_slope_field)
```

```python
import functools

import jax
import jax.numpy as jnp
from jax import lax
from jax.experimental import pallas as pl
from jax.experimental.pallas import tpu as pltpu
from jax.sharding import PartitionSpec as P

SMOOTHING2 = 0.0625
MESH = pl.DeviceIdType.MESH
BF = jnp.bfloat16
F32 = jnp.float32
OP = 72
LANES = 128


def smooth(d):
    return d * lax.rsqrt(d * d + SMOOTHING2)


def lanes_of(shape):
    return lax.broadcasted_iota(jnp.int32, shape, len(shape) - 1)


def exchange_kernel(
    members, lats, lons, rounds, channels,
    xt, wf, off, obs, wv,
    pred, grad, halo_l, halo_r,
    xs, acc, edge, edge_l, edge_r, block, vals, gout, cols, cols_bf,
    xsem, hsend, hrecv, esend, erecv, psend, precv, gsend, grecv, rsend, rrecv, csend, crecv,
):
    me = lax.axis_index("member")
    lat = lax.axis_index("lat")
    lon = lax.axis_index("lon")
    left = lax.rem(lon + lons - 1, lons)
    right = lax.rem(lon + 1, lons)
    rows = rounds * members
    has_up = lat > 0
    has_down = lat < lats - 1

    def chunk_copy(s):
        part = pl.ds(members * s, members)
        return pltpu.make_async_copy(xt.at[part], xs.at[pl.ds(1 + members * s, members)], xsem.at[s])

    for s in (1, 0, 2):
        chunk_copy(s).start()

    barrier = pltpu.get_barrier_semaphore()

    def greet(d, carry):
        pl.semaphore_signal(
            barrier, inc=1, device_id=(lax.rem(me + d, members), lat, lon), device_id_type=MESH
        )
        return carry

    lax.fori_loop(1, members, greet, 0)
    for side in (left, right):
        pl.semaphore_signal(barrier, inc=1, device_id=(me, lat, side), device_id_type=MESH)

    @pl.when(has_up)
    def _():
        pl.semaphore_signal(barrier, inc=1, device_id=(me, lat - 1, lon), device_id_type=MESH)

    @pl.when(has_down)
    def _():
        pl.semaphore_signal(barrier, inc=1, device_id=(me, lat + 1, lon), device_id_type=MESH)

    pl.semaphore_wait(barrier, members - 1 + 2 + has_up.astype(jnp.int32) + has_down.astype(jnp.int32))

    def row_up():
        return pltpu.make_async_remote_copy(
            xt.at[0], xs.at[rows + 1], hsend.at[0], hrecv.at[0],
            device_id=(me, lat - 1, lon), device_id_type=MESH)

    def row_down():
        return pltpu.make_async_remote_copy(
            xt.at[rows - 1], xs.at[0], hsend.at[1], hrecv.at[1],
            device_id=(me, lat + 1, lon), device_id_type=MESH)

    def grow_up():
        return pltpu.make_async_remote_copy(
            grad.at[1], grad.at[rows + 1], rsend.at[0], rrecv.at[0],
            device_id=(me, lat - 1, lon), device_id_type=MESH)

    def grow_down():
        return pltpu.make_async_remote_copy(
            grad.at[rows], grad.at[0], rsend.at[1], rrecv.at[1],
            device_id=(me, lat + 1, lon), device_id_type=MESH)

    @pl.when(has_up)
    def _():
        row_up().start()

    @pl.when(has_down)
    def _():
        row_down().start()

    @pl.when(jnp.logical_not(has_up))
    def _():
        xs[0] = jnp.zeros_like(xs[0])
        grad[0] = jnp.zeros_like(grad[0])

    @pl.when(jnp.logical_not(has_down))
    def _():
        xs[rows + 1] = jnp.zeros_like(xs[rows + 1])
        grad[rows + 1] = jnp.zeros_like(grad[rows + 1])

    lane = lanes_of((OP, LANES))

    def edge_copy(s, side, dst, k):
        return pltpu.make_async_remote_copy(
            edge.at[s], dst.at[s], esend.at[s, k], erecv.at[s, k],
            device_id=(me, lat, side), device_id_type=MESH)

    def convolve(s):
        collected = jnp.zeros((OP, LANES), F32)
        for q in range(members // 2):
            r = members * s + 2 * q
            taps = jnp.concatenate(
                [xs[r:r + 3].reshape(3 * channels, LANES), xs[r + 1:r + 4].reshape(3 * channels, LANES)],
                axis=1)
            res = jnp.dot(wf[...], taps, preferred_element_type=F32)
            for h in range(2):
                i = 2 * q + h
                part = res[:, h * LANES:(h + 1) * LANES]
                a0, a1, a2 = part[:OP], part[OP:2 * OP], part[2 * OP:]
                acc[members * s + i] = (
                    a1
                    + jnp.where(lane == 0, 0.0, pltpu.roll(a0, 1, 1))
                    + jnp.where(lane == LANES - 1, 0.0, pltpu.roll(a2, LANES - 1, 1)))
                collected = jnp.where(lane == i, pltpu.roll(a0, 1 + i, 1), collected)
                mine = a2 if i + 64 == 0 else pltpu.roll(a2, 64 + i, 1)
                collected = jnp.where(lane == 64 + i, mine, collected)
        edge[s] = collected
        edge_copy(s, right, edge_l, 0).start()
        edge_copy(s, left, edge_r, 1).start()

    def pred_copy(s, d, to):
        other = lax.rem(me + d, members) if to else lax.rem(me + members - d, members)
        slot = me if to else other
        return pltpu.make_async_remote_copy(
            pred.at[members * s + other], block.at[s, slot], psend.at[s, d], precv.at[s, slot],
            device_id=(other, lat, lon), device_id_type=MESH)

    def finish(s):
        edge_copy(s, right, edge_l, 0).wait_recv()
        edge_copy(s, left, edge_r, 1).wait_recv()
        for i in range(members):
            from_left = edge_l[s] if i == 0 else pltpu.roll(edge_l[s], LANES - i, 1)
            from_right = pltpu.roll(edge_r[s], 63 - i, 1)
            total = acc[members * s + i] + off[...]
            total = total + jnp.where(lane == 0, from_left, 0.0)
            total = total + jnp.where(lane == LANES - 1, from_right, 0.0)
            pred[members * s + i] = total.astype(BF)

        def send(d, carry):
            pred_copy(s, d, True).start()
            return carry

        lax.fori_loop(1, members, send, 0)
        block[s, me] = pred[members * s + me]

    for s in (1, 0, 2):
        if s == 1:
            for k in range(rounds):
                chunk_copy(k).wait()
        if s == 0:
            @pl.when(has_up)
            def _():
                row_down().wait_recv()
        if s == 2:
            @pl.when(has_down)
            def _():
                row_up().wait_recv()
        convolve(s)
        if s == 0:
            finish(1)
        if s == 2:
            finish(0)
            finish(2)

    def grad_copy(s, d, to):
        other = lax.rem(me + d, members) if to else lax.rem(me + members - d, members)
        owner = me if to else other
        return pltpu.make_async_remote_copy(
            gout.at[s, other], grad.at[1 + members * s + owner], gsend.at[s, d], grecv.at[s, owner],
            device_id=(other, lat, lon), device_id_type=MESH)

    for s in (0, 2, 1):
        def arrive(d, carry):
            pred_copy(s, d, False).wait_recv()
            return carry

        lax.fori_loop(1, members, arrive, 0)
        vals[...] = block[s].astype(F32)

        def slab(k, carry):
            part = pl.ds(pl.multiple_of(8 * k, 8), 8)
            v = vals[:, part, :]
            total = jnp.zeros_like(v)
            for step in range(1, members // 2):
                t = smooth(v - jnp.concatenate([v[step:], v[:step]], axis=0))
                total = total + t - jnp.concatenate([t[members - step:], t[:members - step]], axis=0)
            t = smooth(v[:members // 2] - v[members // 2:])
            total = total + jnp.concatenate([t, -t], axis=0)
            seen = obs[s, part, :].astype(F32)
            vals[:, part, :] = wv[s, part, :] * (smooth(v - seen) - total / (members - 1))
            return carry

        lax.fori_loop(0, OP // 8, slab, 0)
        gout[s] = vals[...].astype(BF)

        def send(d, carry):
            grad_copy(s, d, True).start()
            return carry

        lax.fori_loop(1, members, send, 0)
        grad[1 + members * s + me] = gout[s, me]

    def collect(g):
        row = grad[g].astype(F32)
        now = jnp.where(lane == g, pltpu.roll(row, g, 1), cols[...])
        cols[...] = jnp.where(lane == 64 + g, pltpu.roll(row, 65 + g, 1), now)

    cols[...] = jnp.zeros_like(cols)
    for s in (0, 2, 1):
        def arrive_back(d, carry):
            grad_copy(s, d, False).wait_recv()
            return carry

        lax.fori_loop(1, members, arrive_back, 0)
        if s == 0:
            @pl.when(has_up)
            def _():
                grow_up().start()
        if s == 2:
            @pl.when(has_down)
            def _():
                grow_down().start()

        def gather(i, carry):
            collect(1 + members * s + i)
            return carry

        lax.fori_loop(0, members, gather, 0)

    @pl.when(has_up)
    def _():
        grow_down().wait_recv()

    @pl.when(has_down)
    def _():
        grow_up().wait_recv()

    collect(0)
    collect(rows + 1)
    cols_bf[...] = cols[...].astype(BF)

    def col_copy(side, dst, k):
        return pltpu.make_async_remote_copy(
            cols_bf, dst, csend.at[k], crecv.at[k], device_id=(me, lat, side), device_id_type=MESH)

    col_copy(right, halo_l, 0).start()
    col_copy(left, halo_r, 1).start()

    for s in range(rounds):
        edge_copy(s, right, edge_l, 0).wait_send()
        edge_copy(s, left, edge_r, 1).wait_send()

        def left_device(d, carry):
            pred_copy(s, d, True).wait_send()
            grad_copy(s, d, True).wait_send()
            return carry

        lax.fori_loop(1, members, left_device, 0)

    @pl.when(has_up)
    def _():
        row_up().wait_send()
        grow_up().wait_send()

    @pl.when(has_down)
    def _():
        row_down().wait_send()
        grow_down().wait_send()

    col_copy(right, halo_l, 0).wait()
    col_copy(left, halo_r, 1).wait()


def backward_kernel(block_rows, depth, channels, grad, halo_l, halo_r, wb, out, gs, flat):
    step = pl.program_id(0)
    lane = lanes_of((OP, LANES))
    first = step * block_rows
    hl = halo_l[...].astype(F32)
    hr = halo_r[...].astype(F32)

    def widen(i, carry):
        g = first + i
        row = grad[g].astype(F32)
        after = jnp.where(lane == LANES - 1, pltpu.roll(hr, LANES - 1 - g, 1), pltpu.roll(row, LANES - 1, 1))
        before = jnp.where(lane == 0, pltpu.roll(hl, lax.rem(LANES + 64 - g, LANES), 1), pltpu.roll(row, 1, 1))
        full = jnp.concatenate([after, row, before, jnp.zeros((depth - 3 * OP, LANES), F32)], axis=0)
        gs[i] = full.astype(BF)
        return carry

    lax.fori_loop(0, block_rows + 2, widen, 0)
    for q in range(block_rows // 2):
        r = 2 * q
        taps = jnp.concatenate(
            [gs[r:r + 3].reshape(3 * depth, LANES), gs[r + 1:r + 4].reshape(3 * depth, LANES)], axis=1)
        res = jnp.dot(wb[...], taps, preferred_element_type=F32)
        for h in range(2):
            flat[pl.ds(r + h, channels, stride=block_rows), :] = res[:, h * LANES:(h + 1) * LANES]
    out[...] = flat[...].reshape(channels, block_rows, LANES).astype(BF)


def shards(members, lats, lons, layer_inputs, conv_weight, channel_offset, observed, var_weight):
    channels, rows, cols = layer_inputs.shape[1:]
    outputs = conv_weight.shape[2]
    rounds = rows // members
    total_rows = rows * lats
    depth = 224
    me = lax.axis_index("member")
    lat = lax.axis_index("lat")

    xt = layer_inputs[0].transpose(1, 0, 2)
    weight = jnp.pad(conv_weight, ((0, 0), (0, 0), (0, OP - outputs), (0, 0)))
    wf = weight.transpose(1, 2, 0, 3).reshape(3 * OP, 3 * channels)
    wb = jnp.pad(weight[::-1].reshape(3, 3 * OP, channels), ((0, 0), (0, depth - 3 * OP), (0, 0)))
    wb = wb.reshape(3 * depth, channels).T
    off = jnp.broadcast_to(jnp.pad(channel_offset, (0, OP - outputs))[:, None], (OP, LANES))
    mine = lax.dynamic_index_in_dim(observed.reshape(outputs, rounds, members, cols), me, 2, keepdims=False)
    obs = jnp.pad(mine.transpose(1, 0, 2), ((0, 0), (0, OP - outputs), (0, 0)))
    row_index = (lat * rows + members * jnp.arange(rounds) + me).astype(F32)
    lat_weight = jnp.cos((-80.0 + 160.0 * (row_index + 0.5) / float(total_rows)) * (jnp.pi / 180.0))
    wv = lat_weight[:, None] * jnp.pad(var_weight, (0, OP - outputs))[None, :]
    wv = jnp.broadcast_to(wv[:, :, None], (rounds, OP, LANES))

    vmem = pl.BlockSpec(memory_space=pltpu.VMEM)
    dma = pltpu.SemaphoreType.DMA
    pred, grad, halo_l, halo_r = pl.pallas_call(
        functools.partial(exchange_kernel, members, lats, lons, rounds, channels),
        out_shape=(
            jax.ShapeDtypeStruct((rows, OP, LANES), BF),
            jax.ShapeDtypeStruct((rows + 2, OP, LANES), BF),
            jax.ShapeDtypeStruct((OP, LANES), BF),
            jax.ShapeDtypeStruct((OP, LANES), BF),
        ),
        in_specs=[pl.BlockSpec(memory_space=pl.ANY)] + [vmem] * 4,
        out_specs=(vmem,) * 4,
        scratch_shapes=[
            pltpu.VMEM((rows + 2, channels, LANES), BF),
            pltpu.VMEM((rows, OP, LANES), F32),
            pltpu.VMEM((rounds, OP, LANES), F32),
            pltpu.VMEM((rounds, OP, LANES), F32),
            pltpu.VMEM((rounds, OP, LANES), F32),
            pltpu.VMEM((rounds, members, OP, LANES), BF),
            pltpu.VMEM((members, OP, LANES), F32),
            pltpu.VMEM((rounds, members, OP, LANES), BF),
            pltpu.VMEM((OP, LANES), F32),
            pltpu.VMEM((OP, LANES), BF),
            dma((rounds,)), dma((2,)), dma((2,)), dma((rounds, 2)), dma((rounds, 2)),
            dma((rounds, members)), dma((rounds, members)), dma((rounds, members)), dma((rounds, members)),
            dma((2,)), dma((2,)), dma((2,)), dma((2,)),
        ],
        compiler_params=pltpu.CompilerParams(
            collective_id=0, has_side_effects=True, vmem_limit_bytes=56 * 2**20),
        name="exchange",
    )(xt, wf, off, obs, wv)

    block_rows = 16
    slope = pl.pallas_call(
        functools.partial(backward_kernel, block_rows, depth, channels),
        grid=(rows // block_rows,),
        out_shape=jax.ShapeDtypeStruct((channels, rows, LANES), BF),
        in_specs=[vmem] * 4,
        out_specs=pl.BlockSpec((channels, block_rows, LANES), lambda i: (0, i, 0)),
        scratch_shapes=[
            pltpu.VMEM((block_rows + 2, depth, LANES), BF),
            pltpu.VMEM((channels * block_rows, LANES), F32),
        ],
        compiler_params=pltpu.CompilerParams(vmem_limit_bytes=56 * 2**20),
        name="backward",
    )(grad, halo_l, halo_r, wb)
    return pred[:, :outputs].transpose(1, 0, 2)[None], slope[None]


def solution(mesh):
    members, lats, lons = (mesh.shape[a] for a in ("member", "lat", "lon"))
    in_specs = (P("member", None, "lat", "lon"), P(), P(), P(None, "lat", "lon"), P())
    out_specs = (P("member", None, "lat", "lon"), P("member", None, "lat", "lon"))
    return jax.shard_map(
        functools.partial(shards, members, lats, lons),
        mesh=mesh, in_specs=in_specs, out_specs=out_specs, check_vma=False)
```

```python
import functools
import math

import jax
import jax.numpy as jnp
from jax import lax
from jax.experimental import pallas as pl
from jax.experimental.pallas import tpu as pltpu
from jax.sharding import PartitionSpec as P

SMOOTHING2 = 0.0625
MESH = pl.DeviceIdType.MESH
BF = jnp.bfloat16
F32 = jnp.float32
OP = 72
LANES = 128


def smooth(d):
    return d * lax.rsqrt(d * d + SMOOTHING2)


def lanes_of(shape):
    return lax.broadcasted_iota(jnp.int32, shape, len(shape) - 1)


def column(vector, count):
    rows = lax.broadcasted_iota(jnp.int32, (OP, count), 0)
    spread = jnp.where(rows == lanes_of((OP, count)), jnp.broadcast_to(vector, (OP, count)), 0.0)
    return jnp.broadcast_to(jnp.sum(spread, axis=1, keepdims=True), (OP, LANES))


def exchange_kernel(
    members, lats, lons, rounds, channels, outputs,
    xn, weight, observed, offset_in, var_in,
    pred, grad, halo_l, halo_r, wb,
    xv, xs, stage, wv, wf, obn, obs, offset, var, off, varb, acc, edge, edge_l, edge_r, block, vals, gout, cols, cols_bf,
    xsem, wsem, osem, smem, hsend, hrecv, esend, erecv, psend, precv, gsend, grecv, rsend, rrecv, csend, crecv,
):
    me = lax.axis_index("member")
    lat = lax.axis_index("lat")
    lon = lax.axis_index("lon")
    left = lax.rem(lon + lons - 1, lons)
    right = lax.rem(lon + 1, lons)
    rows = rounds * members
    has_up = lat > 0
    has_down = lat < lats - 1
    blocks = (2, 3, 1, 4, 0, 5)

    def block_copy(j):
        return pltpu.make_async_copy(xn.at[:, pl.ds(8 * j, 8), :], xv.at[j], xsem.at[j])

    def weight_copy():
        return pltpu.make_async_copy(weight, wv, wsem)

    def observed_copy(s):
        start = pl.multiple_of(members * s + 8 * (me // 8), 8)
        return pltpu.make_async_copy(observed.at[:, pl.ds(start, 8), :], obn.at[s], osem.at[s])

    def small_copy(k):
        return pltpu.make_async_copy((offset_in, var_in)[k], (offset, var)[k], smem.at[k])

    for j in blocks[:2]:
        block_copy(j).start()
    weight_copy().start()
    small_copy(0).start()
    small_copy(1).start()
    for j in blocks[2:]:
        block_copy(j).start()
    for s in range(rounds):
        observed_copy(s).start()

    barrier = pltpu.get_barrier_semaphore()

    def greet(d, carry):
        pl.semaphore_signal(
            barrier, inc=1, device_id=(lax.rem(me + d, members), lat, lon), device_id_type=MESH
        )
        return carry

    lax.fori_loop(1, members, greet, 0)
    for side in (left, right):
        pl.semaphore_signal(barrier, inc=1, device_id=(me, lat, side), device_id_type=MESH)

    @pl.when(has_up)
    def _():
        pl.semaphore_signal(barrier, inc=1, device_id=(me, lat - 1, lon), device_id_type=MESH)

    @pl.when(has_down)
    def _():
        pl.semaphore_signal(barrier, inc=1, device_id=(me, lat + 1, lon), device_id_type=MESH)

    def row_up():
        return pltpu.make_async_remote_copy(
            xs.at[1], xs.at[rows + 1], hsend.at[0], hrecv.at[0],
            device_id=(me, lat - 1, lon), device_id_type=MESH)

    def row_down():
        return pltpu.make_async_remote_copy(
            xs.at[rows], xs.at[0], hsend.at[1], hrecv.at[1],
            device_id=(me, lat + 1, lon), device_id_type=MESH)

    def grow_up():
        return pltpu.make_async_remote_copy(
            grad.at[1], grad.at[rows + 1], rsend.at[0], rrecv.at[0],
            device_id=(me, lat - 1, lon), device_id_type=MESH)

    def grow_down():
        return pltpu.make_async_remote_copy(
            grad.at[rows], grad.at[0], rsend.at[1], rrecv.at[1],
            device_id=(me, lat + 1, lon), device_id_type=MESH)

    @pl.when(jnp.logical_not(has_up))
    def _():
        xs[0] = jnp.zeros_like(xs[0])
        grad[0] = jnp.zeros_like(grad[0])

    @pl.when(jnp.logical_not(has_down))
    def _():
        xs[rows + 1] = jnp.zeros_like(xs[rows + 1])
        grad[rows + 1] = jnp.zeros_like(grad[rows + 1])

    lane = lanes_of((OP, LANES))

    def edge_copy(s, side, dst, k):
        return pltpu.make_async_remote_copy(
            edge.at[s], dst.at[s], esend.at[s, k], erecv.at[s, k],
            device_id=(me, lat, side), device_id_type=MESH)

    def convolve(s):
        collected = jnp.zeros((OP, LANES), F32)
        for q in range(members // 2):
            r = members * s + 2 * q
            taps = jnp.concatenate(
                [xs[r:r + 3].reshape(3 * channels, LANES), xs[r + 1:r + 4].reshape(3 * channels, LANES)],
                axis=1)
            res = jnp.dot(wf[...], taps, preferred_element_type=F32)
            for h in range(2):
                i = 2 * q + h
                part = res[:, h * LANES:(h + 1) * LANES]
                a0, a1, a2 = part[:OP], part[OP:2 * OP], part[2 * OP:]
                acc[members * s + i] = (
                    a1
                    + jnp.where(lane == 0, 0.0, pltpu.roll(a0, 1, 1))
                    + jnp.where(lane == LANES - 1, 0.0, pltpu.roll(a2, LANES - 1, 1)))
                collected = jnp.where(lane == i, pltpu.roll(a0, 1 + i, 1), collected)
                mine = a2 if i + 64 == 0 else pltpu.roll(a2, 64 + i, 1)
                collected = jnp.where(lane == 64 + i, mine, collected)
        edge[s] = collected
        edge_copy(s, right, edge_l, 0).start()
        edge_copy(s, left, edge_r, 1).start()

    def pred_copy(s, d, to):
        other = lax.rem(me + d, members) if to else lax.rem(me + members - d, members)
        slot = me if to else other
        return pltpu.make_async_remote_copy(
            pred.at[members * s + other], block.at[s, slot], psend.at[s, d], precv.at[s, slot],
            device_id=(other, lat, lon), device_id_type=MESH)

    def finish(s):
        edge_copy(s, right, edge_l, 0).wait_recv()
        edge_copy(s, left, edge_r, 1).wait_recv()
        for i in range(members):
            from_left = edge_l[s] if i == 0 else pltpu.roll(edge_l[s], LANES - i, 1)
            from_right = pltpu.roll(edge_r[s], 63 - i, 1)
            total = acc[members * s + i] + off[...]
            total = total + jnp.where(lane == 0, from_left, 0.0)
            total = total + jnp.where(lane == LANES - 1, from_right, 0.0)
            pred[members * s + i] = total.astype(BF)

        def send(d, carry):
            pred_copy(s, d, True).start()
            return carry

        lax.fori_loop(1, members, send, 0)
        block[s, me] = pred[members * s + me]

    def relay(j):
        block_copy(j).wait()
        buf = stage.at[j % 2]
        buf[...] = xv[j].astype(F32).reshape(8 * channels, LANES)
        for r in range(8):
            xs[1 + 8 * j + r] = buf[pl.ds(r, channels, stride=8), :].astype(BF)

    weight_copy().wait()
    for a in range(3):
        for b in range(3):
            full = jnp.concatenate(
                [wv[a, b].astype(F32), jnp.zeros((OP - outputs, channels), F32)], axis=0)
            wf[b * OP:(b + 1) * OP, a * channels:(a + 1) * channels] = full.astype(BF)
    small_copy(0).wait()
    off[...] = column(offset[...], outputs)
    for j in blocks[:4]:
        relay(j)
    pl.semaphore_wait(barrier, members - 1 + 2 + has_up.astype(jnp.int32) + has_down.astype(jnp.int32))
    convolve(1)
    relay(0)
    relay(5)
    @pl.when(has_up)
    def _():
        row_up().start()

    @pl.when(has_down)
    def _():
        row_down().start()
    for t in range(3):
        taps = [wv[2 - t, b].astype(F32) for b in range(3)]
        pad = jnp.zeros((OP - outputs, channels), F32)
        tall = jnp.concatenate(
            [taps[0], pad, taps[1], pad, taps[2], pad, jnp.zeros((channels - 3 * OP, channels), F32)], axis=0)
        wb[:, t * channels:(t + 1) * channels] = tall.T.astype(BF)
    finish(1)

    @pl.when(has_up)
    def _():
        row_down().wait_recv()

    convolve(0)

    @pl.when(has_down)
    def _():
        row_up().wait_recv()

    convolve(2)
    finish(0)
    finish(2)

    small_copy(1).wait()
    varb[...] = column(var[...], outputs)
    variable = lax.broadcasted_iota(jnp.int32, (OP, LANES), 0)
    for s in range(rounds):
        observed_copy(s).wait()
        buf = stage.at[s % 2]
        buf[0:8 * outputs, :] = obn[s].astype(F32).reshape(8 * outputs, LANES)
        picked = buf[pl.ds(lax.rem(me, 8), OP, stride=8), :]
        obs[s] = jnp.where(variable < outputs, picked, 0.0)

    def grad_copy(s, d, to):
        other = lax.rem(me + d, members) if to else lax.rem(me + members - d, members)
        owner = me if to else other
        return pltpu.make_async_remote_copy(
            gout.at[s, other], grad.at[1 + members * s + owner], gsend.at[s, d], grecv.at[s, owner],
            device_id=(other, lat, lon), device_id_type=MESH)

    for s in (0, 2, 1):
        def arrive(d, carry):
            pred_copy(s, d, False).wait_recv()
            return carry

        lax.fori_loop(1, members, arrive, 0)
        vals[...] = block[s].astype(F32)
        row_index = jnp.full((8, LANES), lat * rows + members * s + me, jnp.int32).astype(F32)
        angle = -80.0 + 160.0 * (row_index + 0.5) / float(rows * lats)
        lat_weight = jnp.cos(angle * (math.pi / 180.0))

        def slab(k, carry):
            part = pl.ds(pl.multiple_of(8 * k, 8), 8)
            v = vals[:, part, :]
            total = jnp.zeros_like(v)
            for step in range(1, members // 2):
                t = smooth(v - jnp.concatenate([v[step:], v[:step]], axis=0))
                total = total + t - jnp.concatenate([t[members - step:], t[:members - step]], axis=0)
            t = smooth(v[:members // 2] - v[members // 2:])
            total = total + jnp.concatenate([t, -t], axis=0)
            scale = lat_weight * varb[part, :]
            vals[:, part, :] = scale * (smooth(v - obs[s, part, :]) - total / (members - 1))
            return carry

        lax.fori_loop(0, OP // 8, slab, 0)
        gout[s] = vals[...].astype(BF)

        def send(d, carry):
            grad_copy(s, d, True).start()
            return carry

        lax.fori_loop(1, members, send, 0)
        grad[1 + members * s + me] = gout[s, me]

    def collect(g):
        row = grad[g].astype(F32)
        now = jnp.where(lane == g, pltpu.roll(row, g, 1), cols[...])
        cols[...] = jnp.where(lane == 64 + g, pltpu.roll(row, 65 + g, 1), now)

    cols[...] = jnp.zeros_like(cols)
    for s in (0, 2, 1):
        def arrive_back(d, carry):
            grad_copy(s, d, False).wait_recv()
            return carry

        lax.fori_loop(1, members, arrive_back, 0)
        if s == 0:
            @pl.when(has_up)
            def _():
                grow_up().start()
        if s == 2:
            @pl.when(has_down)
            def _():
                grow_down().start()

        def gather(i, carry):
            collect(1 + members * s + i)
            return carry

        lax.fori_loop(0, members, gather, 0)

    @pl.when(has_up)
    def _():
        grow_down().wait_recv()

    @pl.when(has_down)
    def _():
        grow_up().wait_recv()

    collect(0)
    collect(rows + 1)
    cols_bf[...] = cols[...].astype(BF)

    def col_copy(side, dst, k):
        return pltpu.make_async_remote_copy(
            cols_bf, dst, csend.at[k], crecv.at[k], device_id=(me, lat, side), device_id_type=MESH)

    col_copy(right, halo_l, 0).start()
    col_copy(left, halo_r, 1).start()

    for s in range(rounds):
        edge_copy(s, right, edge_l, 0).wait_send()
        edge_copy(s, left, edge_r, 1).wait_send()

        def left_device(d, carry):
            pred_copy(s, d, True).wait_send()
            grad_copy(s, d, True).wait_send()
            return carry

        lax.fori_loop(1, members, left_device, 0)

    @pl.when(has_up)
    def _():
        row_up().wait_send()
        grow_up().wait_send()

    @pl.when(has_down)
    def _():
        row_down().wait_send()
        grow_down().wait_send()

    col_copy(right, halo_l, 0).wait()
    col_copy(left, halo_r, 1).wait()


def backward_kernel(
    block_rows, pitch, channels, outputs, grad, halo_l, halo_r, wb, rows_in, pred, slope, gs, flat, flat_p
):
    step = pl.program_id(0)
    lane = lanes_of((OP, LANES))
    first = step * block_rows
    hl = halo_l[...].astype(F32)
    hr = halo_r[...].astype(F32)
    for i in range(block_rows + 2):
        g = first + i
        row = grad[g].astype(F32)
        after = jnp.where(lane == LANES - 1, pltpu.roll(hr, LANES - 1 - g, 1), pltpu.roll(row, LANES - 1, 1))
        before = jnp.where(lane == 0, pltpu.roll(hl, lax.rem(LANES + 64 - g, LANES), 1), pltpu.roll(row, 1, 1))
        full = jnp.concatenate([after, row, before, jnp.zeros((channels - 3 * OP, LANES), F32)], axis=0)
        gs[i] = full.astype(BF)
    for i in range(block_rows):
        flat_p[pl.ds(i, OP, stride=pitch), :] = rows_in[first + i].astype(F32)
    pred[...] = flat_p[...].reshape(OP, pitch, LANES)[:outputs, :block_rows].astype(BF)
    for q in range(block_rows // 2):
        r = 2 * q
        taps = jnp.concatenate(
            [gs[r:r + 3].reshape(3 * channels, LANES), gs[r + 1:r + 4].reshape(3 * channels, LANES)], axis=1)
        res = jnp.dot(wb[...], taps, preferred_element_type=F32)
        for h in range(2):
            flat[pl.ds(r + h, channels, stride=pitch), :] = res[:, h * LANES:(h + 1) * LANES]
    slope[...] = flat[...].reshape(channels, pitch, LANES)[:, :block_rows].astype(BF)


def shards(members, lats, lons, layer_inputs, conv_weight, channel_offset, observed, var_weight):
    channels, rows = layer_inputs.shape[1:3]
    outputs = conv_weight.shape[2]
    rounds = rows // members

    vmem = pl.BlockSpec(memory_space=pltpu.VMEM)
    hbm = pl.BlockSpec(memory_space=pltpu.HBM)
    dma = pltpu.SemaphoreType.DMA
    per_member = dma((rounds, members))
    pred_rows, grad, halo_l, halo_r, wb = pl.pallas_call(
        functools.partial(exchange_kernel, members, lats, lons, rounds, channels, outputs),
        out_shape=(
            jax.ShapeDtypeStruct((rows, OP, LANES), BF),
            jax.ShapeDtypeStruct((rows + 2, OP, LANES), BF),
            jax.ShapeDtypeStruct((OP, LANES), BF),
            jax.ShapeDtypeStruct((OP, LANES), BF),
            jax.ShapeDtypeStruct((channels, 3 * channels), BF),
        ),
        in_specs=[hbm] * 5,
        out_specs=(vmem,) * 5,
        scratch_shapes=[
            pltpu.VMEM((rows // 8, channels, 8, LANES), BF),
            pltpu.VMEM((rows + 2, channels, LANES), BF),
            pltpu.VMEM((2, 8 * channels, LANES), F32),
            pltpu.VMEM((3, 3, outputs, channels), BF),
            pltpu.VMEM((3 * OP, 3 * channels), BF),
            pltpu.VMEM((rounds, outputs, 8, LANES), BF),
            pltpu.VMEM((rounds, OP, LANES), F32),
            pltpu.VMEM((1, outputs), F32),
            pltpu.VMEM((1, outputs), F32),
            pltpu.VMEM((OP, LANES), F32),
            pltpu.VMEM((OP, LANES), F32),
            pltpu.VMEM((rows, OP, LANES), F32),
            pltpu.VMEM((rounds, OP, LANES), F32),
            pltpu.VMEM((rounds, OP, LANES), F32),
            pltpu.VMEM((rounds, OP, LANES), F32),
            pltpu.VMEM((rounds, members, OP, LANES), BF),
            pltpu.VMEM((members, OP, LANES), F32),
            pltpu.VMEM((rounds, members, OP, LANES), BF),
            pltpu.VMEM((OP, LANES), F32),
            pltpu.VMEM((OP, LANES), BF),
            dma((rows // 8,)), dma, dma((rounds,)), dma((2,)),
            dma((2,)), dma((2,)), dma((rounds, 2)), dma((rounds, 2)),
            per_member, per_member, per_member, per_member,
            dma((2,)), dma((2,)), dma((2,)), dma((2,)),
        ],
        compiler_params=pltpu.CompilerParams(
            collective_id=0, has_side_effects=True, vmem_limit_bytes=67000000),
        name="exchange",
    )(layer_inputs[0], conv_weight, observed, channel_offset[None], var_weight[None])

    block_rows, pitch = 16, 24
    pred, slope = pl.pallas_call(
        functools.partial(backward_kernel, block_rows, pitch, channels, outputs),
        grid=(rows // block_rows,),
        out_shape=(
            jax.ShapeDtypeStruct((outputs, rows, LANES), BF),
            jax.ShapeDtypeStruct((channels, rows, LANES), BF),
        ),
        in_specs=[vmem] * 5,
        out_specs=(
            pl.BlockSpec((outputs, block_rows, LANES), lambda i: (0, i, 0)),
            pl.BlockSpec((channels, block_rows, LANES), lambda i: (0, i, 0)),
        ),
        scratch_shapes=[
            pltpu.VMEM((block_rows + 2, channels, LANES), BF),
            pltpu.VMEM((channels * pitch, LANES), F32),
            pltpu.VMEM((OP * pitch, LANES), F32),
        ],
        compiler_params=pltpu.CompilerParams(vmem_limit_bytes=67000000),
        name="backward",
    )(grad, halo_l, halo_r, wb, pred_rows)
    return pred[None], slope[None]


def solution(mesh):
    members, lats, lons = (mesh.shape[a] for a in ("member", "lat", "lon"))
    in_specs = (P("member", None, "lat", "lon"), P(), P(), P(None, "lat", "lon"), P())
    out_specs = (P("member", None, "lat", "lon"), P("member", None, "lat", "lon"))
    return jax.shard_map(
        functools.partial(shards, members, lats, lons),
        mesh=mesh, in_specs=in_specs, out_specs=out_specs, check_vma=False)
```

```python
import functools
import math

import jax
import jax.numpy as jnp
from jax import lax
from jax.experimental import pallas as pl
from jax.experimental.pallas import tpu as pltpu
from jax.sharding import PartitionSpec as P

SMOOTHING2 = 0.0625
MESH = pl.DeviceIdType.MESH
BF = jnp.bfloat16
F32 = jnp.float32
OP = 72
LANES = 128


def smooth(d):
    return d * lax.rsqrt(d * d + SMOOTHING2)


def lanes_of(shape):
    return lax.broadcasted_iota(jnp.int32, shape, len(shape) - 1)


def column(vector, count):
    rows = lax.broadcasted_iota(jnp.int32, (OP, count), 0)
    spread = jnp.where(rows == lanes_of((OP, count)), jnp.broadcast_to(vector, (OP, count)), 0.0)
    return jnp.broadcast_to(jnp.sum(spread, axis=1, keepdims=True), (OP, LANES))


def beyond_columns(grad, indices, outputs, stage):
    last = OP - 8
    for g in indices:
        stage[8 * g:8 * g + 8, :] = grad[g, last:OP, :].astype(F32)
    to_left = stage[pl.ds(outputs - last, 64, stride=8), :]
    to_right = stage[pl.ds(outputs - last + 1, 64, stride=8), :]
    return jnp.concatenate([to_left, to_right], axis=0).T[:OP]


def widen(grad, g, sides, at, channels):
    lane = lanes_of((OP, LANES))
    row = grad[g].astype(F32)
    right = pltpu.roll(sides, (63 - at) % LANES, 1)
    left = sides if at == 0 else pltpu.roll(sides, LANES - at, 1)
    after = jnp.where(lane == LANES - 1, right, pltpu.roll(row, LANES - 1, 1))
    before = jnp.where(lane == 0, left, pltpu.roll(row, 1, 1))
    return jnp.concatenate(
        [after, row, before, jnp.zeros((channels - 3 * OP, LANES), F32)], axis=0).astype(BF)


def slope_rows(wb, gs, flat, starts, shift, pitch, channels):
    for r in starts:
        taps = jnp.concatenate(
            [gs[r:r + 3].reshape(3 * channels, LANES), gs[r + 1:r + 4].reshape(3 * channels, LANES)], axis=1)
        res = jnp.dot(wb[...], taps, preferred_element_type=F32)
        for h in range(2):
            flat[pl.ds(r + h + shift, channels, stride=pitch), :] = res[:, h * LANES:(h + 1) * LANES]


def exchange_kernel(
    members, lats, lons, rounds, channels, outputs,
    xn, weight, observed, offset_in, var_in,
    pred_out, grad, wb, slope_out,
    xv, xs, stage, wv, wf, obn, obs, offset, var, off, varb, acc, edge, edge_l, edge_r, block, vals, gout, gcol, gcol_l, gcol_r, pred, gs, flat, flat_p, pbuf, sbuf,
    xsem, wsem, osem, smem, hsend, hrecv, esend, erecv, psend, precv, gsend, grecv, rsend, rrecv, csend, crecv, fsem,
):
    me = lax.axis_index("member")
    lat = lax.axis_index("lat")
    lon = lax.axis_index("lon")
    left = lax.rem(lon + lons - 1, lons)
    right = lax.rem(lon + 1, lons)
    rows = rounds * members
    has_up = lat > 0
    has_down = lat < lats - 1
    blocks = (2, 3, 1, 4, 0, 5)

    def block_copy(j):
        return pltpu.make_async_copy(xn.at[:, pl.ds(8 * j, 8), :], xv.at[j], xsem.at[j])

    def weight_copy():
        return pltpu.make_async_copy(weight, wv, wsem)

    def observed_copy(s):
        start = pl.multiple_of(members * s + 8 * (me // 8), 8)
        return pltpu.make_async_copy(observed.at[:, pl.ds(start, 8), :], obn.at[s], osem.at[s])

    def small_copy(k):
        return pltpu.make_async_copy((offset_in, var_in)[k], (offset, var)[k], smem.at[k])

    for j in blocks[:2]:
        block_copy(j).start()
    weight_copy().start()
    small_copy(0).start()
    small_copy(1).start()
    for j in blocks[2:]:
        block_copy(j).start()
    for s in range(rounds):
        observed_copy(s).start()

    barrier = pltpu.get_barrier_semaphore()

    def greet(d, carry):
        pl.semaphore_signal(
            barrier, inc=1, device_id=(lax.rem(me + d, members), lat, lon), device_id_type=MESH
        )
        return carry

    lax.fori_loop(1, members, greet, 0)
    for side in (left, right):
        pl.semaphore_signal(barrier, inc=1, device_id=(me, lat, side), device_id_type=MESH)

    @pl.when(has_up)
    def _():
        pl.semaphore_signal(barrier, inc=1, device_id=(me, lat - 1, lon), device_id_type=MESH)

    @pl.when(has_down)
    def _():
        pl.semaphore_signal(barrier, inc=1, device_id=(me, lat + 1, lon), device_id_type=MESH)

    def row_up():
        return pltpu.make_async_remote_copy(
            xs.at[1], xs.at[rows + 1], hsend.at[0], hrecv.at[0],
            device_id=(me, lat - 1, lon), device_id_type=MESH)

    def row_down():
        return pltpu.make_async_remote_copy(
            xs.at[rows], xs.at[0], hsend.at[1], hrecv.at[1],
            device_id=(me, lat + 1, lon), device_id_type=MESH)

    def grow_up():
        return pltpu.make_async_remote_copy(
            grad.at[1], grad.at[rows + 1], rsend.at[0], rrecv.at[0],
            device_id=(me, lat - 1, lon), device_id_type=MESH)

    def grow_down():
        return pltpu.make_async_remote_copy(
            grad.at[rows], grad.at[0], rsend.at[1], rrecv.at[1],
            device_id=(me, lat + 1, lon), device_id_type=MESH)

    @pl.when(jnp.logical_not(has_up))
    def _():
        xs[0] = jnp.zeros_like(xs[0])
        grad[0] = jnp.zeros_like(grad[0])

    @pl.when(jnp.logical_not(has_down))
    def _():
        xs[rows + 1] = jnp.zeros_like(xs[rows + 1])
        grad[rows + 1] = jnp.zeros_like(grad[rows + 1])

    lane = lanes_of((OP, LANES))

    def edge_copy(s, side, dst, k):
        return pltpu.make_async_remote_copy(
            edge.at[s], dst.at[s], esend.at[s, k], erecv.at[s, k],
            device_id=(me, lat, side), device_id_type=MESH)

    def convolve(s):
        collected = jnp.zeros((OP, LANES), F32)
        for q in range(members // 2):
            r = members * s + 2 * q
            taps = jnp.concatenate(
                [xs[r:r + 3].reshape(3 * channels, LANES), xs[r + 1:r + 4].reshape(3 * channels, LANES)],
                axis=1)
            res = jnp.dot(wf[...], taps, preferred_element_type=F32)
            for h in range(2):
                i = 2 * q + h
                part = res[:, h * LANES:(h + 1) * LANES]
                a0, a1, a2 = part[:OP], part[OP:2 * OP], part[2 * OP:]
                acc[members * s + i] = (
                    a1
                    + jnp.where(lane == 0, 0.0, pltpu.roll(a0, 1, 1))
                    + jnp.where(lane == LANES - 1, 0.0, pltpu.roll(a2, LANES - 1, 1)))
                collected = jnp.where(lane == i, pltpu.roll(a0, 1 + i, 1), collected)
                mine = a2 if i + 64 == 0 else pltpu.roll(a2, 64 + i, 1)
                collected = jnp.where(lane == 64 + i, mine, collected)
        edge[s] = collected

    def send_edges(s):
        edge_copy(s, right, edge_l, 0).start()
        edge_copy(s, left, edge_r, 1).start()

    def pred_copy(s, d, to):
        other = lax.rem(me + d, members) if to else lax.rem(me + members - d, members)
        slot = me if to else other
        return pltpu.make_async_remote_copy(
            pred.at[members * s + other], block.at[s, slot], psend.at[s, d], precv.at[s, slot],
            device_id=(other, lat, lon), device_id_type=MESH)

    def finish(s):
        edge_copy(s, right, edge_l, 0).wait_recv()
        edge_copy(s, left, edge_r, 1).wait_recv()
        for i in range(members):
            from_left = edge_l[s] if i == 0 else pltpu.roll(edge_l[s], LANES - i, 1)
            from_right = pltpu.roll(edge_r[s], 63 - i, 1)
            total = acc[members * s + i] + off[...]
            total = total + jnp.where(lane == 0, from_left, 0.0)
            total = total + jnp.where(lane == LANES - 1, from_right, 0.0)
            pred[members * s + i] = total.astype(BF)

        def send(d, carry):
            pred_copy(s, d, True).start()
            return carry

        lax.fori_loop(1, members, send, 0)
        block[s, me] = pred[members * s + me]

    def relay(j):
        block_copy(j).wait()
        buf = stage.at[j % 2]
        buf[...] = xv[j].astype(F32).reshape(8 * channels, LANES)
        for r in range(8):
            xs[1 + 8 * j + r] = buf[pl.ds(r, channels, stride=8), :].astype(BF)

    weight_copy().wait()
    for a in range(3):
        for b in range(3):
            full = jnp.concatenate(
                [wv[a, b].astype(F32), jnp.zeros((OP - outputs, channels), F32)], axis=0)
            wf[b * OP:(b + 1) * OP, a * channels:(a + 1) * channels] = full.astype(BF)
    small_copy(0).wait()
    off[...] = column(offset[...], outputs)
    for j in blocks[:4]:
        relay(j)
    convolve(1)
    pl.semaphore_wait(barrier, members - 1 + 2 + has_up.astype(jnp.int32) + has_down.astype(jnp.int32))
    send_edges(1)
    relay(0)
    relay(5)
    @pl.when(has_up)
    def _():
        row_up().start()

    @pl.when(has_down)
    def _():
        row_down().start()

    for t in range(3):
        taps = [wv[2 - t, b].astype(F32) for b in range(3)]
        pad = jnp.zeros((OP - outputs, channels), F32)
        tall = jnp.concatenate(
            [taps[0], pad, taps[1], pad, taps[2], pad, jnp.zeros((channels - 3 * OP, channels), F32)], axis=0)
        wb[:, t * channels:(t + 1) * channels] = tall.T.astype(BF)
    finish(1)

    @pl.when(has_up)
    def _():
        row_down().wait_recv()

    convolve(0)
    send_edges(0)

    @pl.when(has_down)
    def _():
        row_up().wait_recv()

    convolve(2)
    send_edges(2)
    finish(0)
    finish(2)

    small_copy(1).wait()
    varb[...] = column(var[...], outputs)
    variable = lax.broadcasted_iota(jnp.int32, (OP, LANES), 0)
    for s in range(rounds):
        observed_copy(s).wait()
        buf = stage.at[s % 2]
        buf[0:8 * outputs, :] = obn[s].astype(F32).reshape(8 * outputs, LANES)
        picked = buf[pl.ds(lax.rem(me, 8), OP, stride=8), :]
        obs[s] = jnp.where(variable < outputs, picked, 0.0)

    def col_copy(s, side, dst, k):
        return pltpu.make_async_remote_copy(
            gcol.at[s], dst.at[s], csend.at[s, k], crecv.at[s, k],
            device_id=(me, lat, side), device_id_type=MESH)

    def grad_copy(s, d, to):
        other = lax.rem(me + d, members) if to else lax.rem(me + members - d, members)
        owner = me if to else other
        return pltpu.make_async_remote_copy(
            gout.at[s, other], grad.at[1 + members * s + owner], gsend.at[s, d], grecv.at[s, owner],
            device_id=(other, lat, lon), device_id_type=MESH)

    for s in (0, 2, 1):
        def arrive(d, carry):
            pred_copy(s, d, False).wait_recv()
            return carry

        lax.fori_loop(1, members, arrive, 0)
        vals[...] = block[s].astype(F32)
        row_index = jnp.full((8, LANES), lat * rows + members * s + me, jnp.int32).astype(F32)
        angle = -80.0 + 160.0 * (row_index + 0.5) / float(rows * lats)
        lat_weight = jnp.cos(angle * (math.pi / 180.0))

        def slab(k, carry):
            part = pl.ds(pl.multiple_of(8 * k, 8), 8)
            v = vals[:, part, :]
            total = jnp.zeros_like(v)
            for step in range(1, members // 2):
                t = smooth(v - jnp.concatenate([v[step:], v[:step]], axis=0))
                total = total + t - jnp.concatenate([t[members - step:], t[:members - step]], axis=0)
            t = smooth(v[:members // 2] - v[members // 2:])
            total = total + jnp.concatenate([t, -t], axis=0)
            scale = lat_weight * varb[part, :]
            vals[:, part, :] = scale * (smooth(v - obs[s, part, :]) - total / (members - 1))
            return carry

        lax.fori_loop(0, OP // 8, slab, 0)
        collected = jnp.zeros((OP, LANES), F32)
        for j in range(members):
            first = vals[j] if j == 0 else pltpu.roll(vals[j], j, 1)
            collected = jnp.where(lane == j, first, collected)
            collected = jnp.where(lane == 64 + j, pltpu.roll(vals[j], 65 + j, 1), collected)
        gcol[s] = collected.astype(BF)
        col_copy(s, right, gcol_l, 0).start()
        col_copy(s, left, gcol_r, 1).start()
        col_copy(s, right, gcol_l, 0).wait_recv()
        col_copy(s, left, gcol_r, 1).wait_recv()
        both = jnp.where(
            lane < 64, pltpu.roll(gcol_l[s].astype(F32), 64, 1), pltpu.roll(gcol_r[s].astype(F32), 64, 1))
        across = jnp.concatenate([both, jnp.zeros((LANES - OP, LANES), F32)], axis=0).T
        for j in range(members):
            vals[j, outputs:outputs + 1, :] = across[j:j + 1]
            vals[j, outputs + 1:outputs + 2, :] = across[64 + j:65 + j]
        gout[s] = vals[...].astype(BF)

        def send(d, carry):
            grad_copy(s, d, True).start()
            return carry

        lax.fori_loop(1, members, send, 0)
        grad[1 + members * s + me] = gout[s, me]

    def return_of(s):
        def arrive_back(d, carry):
            grad_copy(s, d, False).wait_recv()
            return carry

        lax.fori_loop(1, members, arrive_back, 0)

    def pred_part(s):
        for i in range(members):
            flat_p[pl.ds(i, OP, stride=24), :] = pred[members * s + i].astype(F32)
        pbuf[s] = flat_p[...].reshape(OP, 24, LANES)[:outputs, :members].astype(BF)

    def pred_done(s):
        return pltpu.make_async_copy(pbuf.at[s], pred_out.at[:, pl.ds(members * s, members), :], fsem.at[s])

    for s in range(rounds):
        pred_part(s)
        pred_done(s).start()

    return_of(0)

    @pl.when(has_up)
    def _():
        grow_up().start()

    return_of(2)

    @pl.when(has_down)
    def _():
        grow_down().start()

    @pl.when(has_up)
    def _():
        grow_down().wait_recv()

    @pl.when(has_down)
    def _():
        grow_up().wait_recv()

    def slope_copy(k):
        return pltpu.make_async_copy(
            sbuf.at[k], slope_out.at[:, pl.ds(2 * members * k, members), :], fsem.at[rounds + k])

    early = (range(0, members + 1), range(2 * members + 1, rows + 2))
    sides = beyond_columns(grad, [*early[0], *early[1]], outputs, stage.at[0])
    starts = [*range(0, members - 3, 2), members - 3]
    for k, part in enumerate(early):
        for i, g in enumerate(part):
            gs[k, i] = widen(grad, g, sides, g, channels)
        slope_rows(wb, gs.at[k], flat.at[k], starts, k, 24, channels)
        sbuf[k] = flat[k].reshape(channels, 24, LANES)[:, :members].astype(BF)
        slope_copy(k).start()

    return_of(1)

    for s in range(rounds):
        edge_copy(s, right, edge_l, 0).wait_send()
        edge_copy(s, left, edge_r, 1).wait_send()
        col_copy(s, right, gcol_l, 0).wait_send()
        col_copy(s, left, gcol_r, 1).wait_send()

        def left_device(d, carry):
            pred_copy(s, d, True).wait_send()
            grad_copy(s, d, True).wait_send()
            return carry

        lax.fori_loop(1, members, left_device, 0)

    @pl.when(has_up)
    def _():
        row_up().wait_send()
        grow_up().wait_send()

    @pl.when(has_down)
    def _():
        row_down().wait_send()
        grow_down().wait_send()

    for s in range(rounds):
        pred_done(s).wait()
    for k in range(2):
        slope_copy(k).wait()


def backward_kernel(
    members, channels, outputs, grad_in, wb_in, slope_in, pred_in, pred, slope,
    grad, wb, blocks, pbuf, gs, flat, stage, isem, osem,
):
    count = members + 4
    first = members - 1
    pitch = 2 * members + 8
    ins = [
        pltpu.make_async_copy(grad_in.at[pl.ds(first, count)], grad, isem.at[0]),
        pltpu.make_async_copy(wb_in, wb, isem.at[1]),
    ]
    block_at = (0, 1, 4, 5)
    for k, j in enumerate(block_at):
        ins.append(pltpu.make_async_copy(slope_in.at[:, pl.ds(8 * j, 8), :], blocks.at[j], isem.at[2 + k]))
    ins.append(pltpu.make_async_copy(pred_in, pbuf, isem.at[6]))
    for c in ins:
        c.start()

    def out_copy(j):
        return pltpu.make_async_copy(blocks.at[j], slope.at[:, pl.ds(8 * j, 8), :], osem.at[j])

    pred_copy = pltpu.make_async_copy(pbuf, pred, osem.at[6])
    ins[0].wait()
    sides = beyond_columns(grad, range(count), outputs, stage)
    for i in range(count):
        gs[i] = widen(grad, i, sides, i, channels)
    ins[1].wait()
    for k, j in ((2, 0), (5, 5)):
        ins[k].wait()
        out_copy(j).start()
    ins[6].wait()
    pred_copy.start()
    slope_rows(wb, gs, flat, range(0, members + 2, 2), 7, pitch, channels)
    ins[3].wait()
    ins[4].wait()
    area = (channels, 8, LANES)
    row = lax.broadcasted_iota(jnp.int32, area, 1)
    new = flat[...].reshape(channels, pitch, LANES)
    for j in (2, 3):
        blocks[j] = new[:, 8 * j - 8:8 * j].astype(BF)
        out_copy(j).start()
    blocks[1] = jnp.where(row == 7, new[:, 0:8], blocks[1].astype(F32)).astype(BF)
    out_copy(1).start()
    blocks[4] = jnp.where(row == 0, new[:, 24:32], blocks[4].astype(F32)).astype(BF)
    out_copy(4).start()
    for j in range(6):
        out_copy(j).wait()
    pred_copy.wait()


def shards(members, lats, lons, layer_inputs, conv_weight, channel_offset, observed, var_weight):
    channels, rows = layer_inputs.shape[1:3]
    outputs = conv_weight.shape[2]
    rounds = rows // members

    vmem = pl.BlockSpec(memory_space=pltpu.VMEM)
    hbm = pl.BlockSpec(memory_space=pltpu.HBM)
    dma = pltpu.SemaphoreType.DMA
    per_member = dma((rounds, members))
    pred_a, grad, wb, slope_a = pl.pallas_call(
        functools.partial(exchange_kernel, members, lats, lons, rounds, channels, outputs),
        out_shape=(
            jax.ShapeDtypeStruct((outputs, rows, LANES), BF),
            jax.ShapeDtypeStruct((rows + 2, OP, LANES), BF),
            jax.ShapeDtypeStruct((channels, 3 * channels), BF),
            jax.ShapeDtypeStruct((channels, rows, LANES), BF),
        ),
        in_specs=[hbm] * 5,
        out_specs=(hbm, vmem, vmem, hbm),
        scratch_shapes=[
            pltpu.VMEM((rows // 8, channels, 8, LANES), BF),
            pltpu.VMEM((rows + 2, channels, LANES), BF),
            pltpu.VMEM((2, 8 * channels, LANES), F32),
            pltpu.VMEM((3, 3, outputs, channels), BF),
            pltpu.VMEM((3 * OP, 3 * channels), BF),
            pltpu.VMEM((rounds, outputs, 8, LANES), BF),
            pltpu.VMEM((rounds, OP, LANES), F32),
            pltpu.VMEM((1, outputs), F32),
            pltpu.VMEM((1, outputs), F32),
            pltpu.VMEM((OP, LANES), F32),
            pltpu.VMEM((OP, LANES), F32),
            pltpu.VMEM((rows, OP, LANES), F32),
            pltpu.VMEM((rounds, OP, LANES), F32),
            pltpu.VMEM((rounds, OP, LANES), F32),
            pltpu.VMEM((rounds, OP, LANES), F32),
            pltpu.VMEM((rounds, members, OP, LANES), BF),
            pltpu.VMEM((members, OP, LANES), F32),
            pltpu.VMEM((rounds, members, OP, LANES), BF),
            pltpu.VMEM((rounds, OP, LANES), BF),
            pltpu.VMEM((rounds, OP, LANES), BF),
            pltpu.VMEM((rounds, OP, LANES), BF),
            pltpu.VMEM((rows, OP, LANES), BF),
            pltpu.VMEM((2, members + 2, channels, LANES), BF),
            pltpu.VMEM((2, channels * 24, LANES), F32),
            pltpu.VMEM((OP * 24, LANES), F32),
            pltpu.VMEM((rounds, outputs, members, LANES), BF),
            pltpu.VMEM((2, channels, members, LANES), BF),
            dma((rows // 8,)), dma, dma((rounds,)), dma((2,)),
            dma((2,)), dma((2,)), dma((rounds, 2)), dma((rounds, 2)),
            per_member, per_member, per_member, per_member,
            dma((2,)), dma((2,)), dma((rounds, 2)), dma((rounds, 2)), dma((rounds + 2,)),
        ],
        compiler_params=pltpu.CompilerParams(
            collective_id=0, has_side_effects=True, vmem_limit_bytes=67000000),
        name="exchange",
    )(layer_inputs[0], conv_weight, observed, channel_offset[None], var_weight[None])

    pred, slope = pl.pallas_call(
        functools.partial(backward_kernel, members, channels, outputs),
        out_shape=(
            jax.ShapeDtypeStruct((outputs, rows, LANES), BF),
            jax.ShapeDtypeStruct((channels, rows, LANES), BF),
        ),
        in_specs=[hbm] * 4,
        out_specs=(hbm, hbm),
        scratch_shapes=[
            pltpu.VMEM((members + 4, OP, LANES), BF),
            pltpu.VMEM((channels, 3 * channels), BF),
            pltpu.VMEM((rows // 8, channels, 8, LANES), BF),
            pltpu.VMEM((outputs, rows, LANES), BF),
            pltpu.VMEM((members + 4, channels, LANES), BF),
            pltpu.VMEM((channels * (2 * members + 8), LANES), F32),
            pltpu.VMEM((8 * 64, LANES), F32),
            dma((7,)), dma((7,)),
        ],
        compiler_params=pltpu.CompilerParams(vmem_limit_bytes=67000000),
        name="backward",
    )(grad, wb, slope_a, pred_a)
    return pred[None], slope[None]


def solution(mesh):
    members, lats, lons = (mesh.shape[a] for a in ("member", "lat", "lon"))
    in_specs = (P("member", None, "lat", "lon"), P(), P(), P(None, "lat", "lon"), P())
    out_specs = (P("member", None, "lat", "lon"), P("member", None, "lat", "lon"))
    return jax.shard_map(
        functools.partial(shards, members, lats, lons),
        mesh=mesh, in_specs=in_specs, out_specs=out_specs, check_vma=False)
```

```python
import functools
import math

import jax
import jax.numpy as jnp
from jax import lax
from jax.experimental import pallas as pl
from jax.experimental.pallas import tpu as pltpu
from jax.sharding import PartitionSpec as P

SMOOTHING2 = 0.0625
MESH = pl.DeviceIdType.MESH
BF = jnp.bfloat16
F32 = jnp.float32
OP = 72
LANES = 128


def smooth(d):
    return d * lax.rsqrt(d * d + SMOOTHING2)


def lanes_of(shape):
    return lax.broadcasted_iota(jnp.int32, shape, len(shape) - 1)


def rounds_of(members, rows):
    m = members
    return (
        [*range(1, m - 1), 2 * m + 1, 2 * m + 2],
        [0, m - 1, 2 * m, *range(2 * m + 3, rows)],
        [*range(m, 2 * m)],
    )


def row_at(plan, s, owner):
    listed, members = plan[s], len(plan[s])
    row = owner + listed[0]
    for k in range(1, members):
        jump = listed[k] - listed[k - 1] - 1
        if jump:
            row = row + jump * ((owner + members - k) // members)
    return row


def column(vector, count):
    rows = lax.broadcasted_iota(jnp.int32, (OP, count), 0)
    spread = jnp.where(rows == lanes_of((OP, count)), jnp.broadcast_to(vector, (OP, count)), 0.0)
    return jnp.broadcast_to(jnp.sum(spread, axis=1, keepdims=True), (OP, LANES))


def beyond_columns(grad, indices, outputs, stage):
    last = OP - 8
    for g in indices:
        stage[8 * g:8 * g + 8, :] = grad[g, last:OP, :].astype(F32)
    to_left = stage[pl.ds(outputs - last, 64, stride=8), :]
    to_right = stage[pl.ds(outputs - last + 1, 64, stride=8), :]
    return jnp.concatenate([to_left, to_right], axis=0).T[:OP]


def widen(grad, g, sides, at, channels):
    lane = lanes_of((OP, LANES))
    row = grad[g].astype(F32)
    right = pltpu.roll(sides, (63 - at) % LANES, 1)
    left = sides if at == 0 else pltpu.roll(sides, LANES - at, 1)
    after = jnp.where(lane == LANES - 1, right, pltpu.roll(row, LANES - 1, 1))
    before = jnp.where(lane == 0, left, pltpu.roll(row, 1, 1))
    return jnp.concatenate(
        [after, row, before, jnp.zeros((channels - 3 * OP, LANES), F32)], axis=0).astype(BF)


def slope_rows(wb, gs, flat, starts, shift, pitch, channels):
    for r in starts:
        taps = jnp.concatenate(
            [gs[r:r + 3].reshape(3 * channels, LANES), gs[r + 1:r + 4].reshape(3 * channels, LANES)], axis=1)
        res = jnp.dot(wb[...], taps, preferred_element_type=F32)
        for h in range(2):
            flat[pl.ds(r + h + shift, channels, stride=pitch), :] = res[:, h * LANES:(h + 1) * LANES]


def exchange_kernel(
    members, lats, lons, rounds, channels, outputs,
    xn, weight, observed, offset_in, var_in,
    pred_out, grad_out, wb_out, slope_out,
    xv, xs, stage, wv, wf, obn, obs, offset, var, off, varb, acc, edge, edge_l, edge_r, block, vals_of, gout, gcol, gcol_l, gcol_r, pred, gs, flat, flat_p, pbuf, sbuf, grad, wb,
    xsem, wsem, osem, smem, hsend, hrecv, esend, erecv, psend, precv, gsend, grecv, rsend, rrecv, csend, crecv, fsem, ready,
):
    me = lax.axis_index("member")
    lat = lax.axis_index("lat")
    lon = lax.axis_index("lon")
    left = lax.rem(lon + lons - 1, lons)
    right = lax.rem(lon + 1, lons)
    rows = rounds * members
    has_up = lat > 0
    has_down = lat < lats - 1
    plan = rounds_of(members, rows)
    blocks = (0, 1, 4, 2, 3, 5)
    mine = [row_at(plan, s, me) for s in range(rounds)]

    def block_copy(j):
        return pltpu.make_async_copy(xn.at[:, pl.ds(8 * j, 8), :], xv.at[j], xsem.at[j])

    def weight_copy():
        return pltpu.make_async_copy(weight, wv, wsem)

    def observed_copy(s):
        start = pl.multiple_of(8 * (mine[s] // 8), 8)
        return pltpu.make_async_copy(observed.at[:, pl.ds(start, 8), :], obn.at[s], osem.at[s])

    def small_copy(k):
        return pltpu.make_async_copy((offset_in, var_in)[k], (offset, var)[k], smem.at[k])

    for j in blocks[:2]:
        block_copy(j).start()
    weight_copy().start()
    small_copy(0).start()
    small_copy(1).start()
    for j in blocks[2:]:
        block_copy(j).start()
    for s in range(rounds):
        observed_copy(s).start()

    barrier = pltpu.get_barrier_semaphore()

    side_len = math.isqrt(members)
    own_col, own_row = me // side_len, lax.rem(me, side_len)

    def in_row(d):
        return (own_col * side_len + lax.rem(own_row + d, side_len), lat, lon)

    for d in range(1, side_len):
        pl.semaphore_signal(barrier, inc=1, device_id=in_row(d), device_id_type=MESH)
        pl.semaphore_signal(
            barrier, inc=1, device_id=(lax.rem(me + d * side_len, members), lat, lon), device_id_type=MESH)
    for side in (left, right):
        pl.semaphore_signal(barrier, inc=1, device_id=(me, lat, side), device_id_type=MESH)

    @pl.when(has_up)
    def _():
        pl.semaphore_signal(barrier, inc=1, device_id=(me, lat - 1, lon), device_id_type=MESH)

    @pl.when(has_down)
    def _():
        pl.semaphore_signal(barrier, inc=1, device_id=(me, lat + 1, lon), device_id_type=MESH)

    def row_up():
        return pltpu.make_async_remote_copy(
            xs.at[1], xs.at[rows + 1], hsend.at[0], hrecv.at[0],
            device_id=(me, lat - 1, lon), device_id_type=MESH)

    def row_down():
        return pltpu.make_async_remote_copy(
            xs.at[rows], xs.at[0], hsend.at[1], hrecv.at[1],
            device_id=(me, lat + 1, lon), device_id_type=MESH)

    def grow_up():
        return pltpu.make_async_remote_copy(
            grad.at[1], grad.at[rows + 1], rsend.at[0], rrecv.at[0],
            device_id=(me, lat - 1, lon), device_id_type=MESH)

    def grow_down():
        return pltpu.make_async_remote_copy(
            grad.at[rows], grad.at[0], rsend.at[1], rrecv.at[1],
            device_id=(me, lat + 1, lon), device_id_type=MESH)

    @pl.when(jnp.logical_not(has_up))
    def _():
        xs[0] = jnp.zeros_like(xs[0])
        grad[0] = jnp.zeros_like(grad[0])

    @pl.when(jnp.logical_not(has_down))
    def _():
        xs[rows + 1] = jnp.zeros_like(xs[rows + 1])
        grad[rows + 1] = jnp.zeros_like(grad[rows + 1])

    lane = lanes_of((OP, LANES))

    def edge_copy(s, side, dst, k):
        return pltpu.make_async_remote_copy(
            edge.at[s], dst.at[s], esend.at[s, k], erecv.at[s, k],
            device_id=(me, lat, side), device_id_type=MESH)

    def convolve(s):
        collected = jnp.zeros((OP, LANES), F32)
        for q in range(members // 2):
            taps = jnp.concatenate(
                [xs[r:r + 3].reshape(3 * channels, LANES) for r in plan[s][2 * q:2 * q + 2]], axis=1)
            res = jnp.dot(wf[...], taps, preferred_element_type=F32)
            for h in range(2):
                i = 2 * q + h
                part = res[:, h * LANES:(h + 1) * LANES]
                a0, a1, a2 = part[:OP], part[OP:2 * OP], part[2 * OP:]
                acc[members * s + i] = (
                    a1
                    + jnp.where(lane == 0, 0.0, pltpu.roll(a0, 1, 1))
                    + jnp.where(lane == LANES - 1, 0.0, pltpu.roll(a2, LANES - 1, 1)))
                collected = jnp.where(lane == i, pltpu.roll(a0, 1 + i, 1), collected)
                mine = a2 if i + 64 == 0 else pltpu.roll(a2, 64 + i, 1)
                collected = jnp.where(lane == 64 + i, mine, collected)
        edge[s] = collected

    def send_edges(s):
        edge_copy(s, right, edge_l, 0).start()
        edge_copy(s, left, edge_r, 1).start()

    def pred_copy(s, d, to):
        other = lax.rem(me + d, members) if to else lax.rem(me + members - d, members)
        slot = me if to else other
        return pltpu.make_async_remote_copy(
            pred.at[members * s + other], block.at[s, slot], psend.at[s, d], precv.at[s, slot],
            device_id=(other, lat, lon), device_id_type=MESH)

    def finish(s):
        edge_copy(s, right, edge_l, 0).wait_recv()
        edge_copy(s, left, edge_r, 1).wait_recv()
        for i in range(members):
            from_left = edge_l[s] if i == 0 else pltpu.roll(edge_l[s], LANES - i, 1)
            from_right = pltpu.roll(edge_r[s], 63 - i, 1)
            total = acc[members * s + i] + off[...]
            total = total + jnp.where(lane == 0, from_left, 0.0)
            total = total + jnp.where(lane == LANES - 1, from_right, 0.0)
            pred[members * s + i] = total.astype(BF)

        def send(d, carry):
            pred_copy(s, d, True).start()
            return carry

        lax.fori_loop(1, members, send, 0)
        block[s, me] = pred[members * s + me]

    def relay(j):
        block_copy(j).wait()
        buf = stage.at[j % 2]
        buf[...] = xv[j].astype(F32).reshape(8 * channels, LANES)
        for r in range(8):
            xs[1 + 8 * j + r] = buf[pl.ds(r, channels, stride=8), :].astype(BF)

    weight_copy().wait()
    for a in range(3):
        for b in range(3):
            full = jnp.concatenate(
                [wv[a, b].astype(F32), jnp.zeros((OP - outputs, channels), F32)], axis=0)
            wf[b * OP:(b + 1) * OP, a * channels:(a + 1) * channels] = full.astype(BF)
    small_copy(0).wait()
    off[...] = column(offset[...], outputs)
    for j in blocks[:3]:
        relay(j)
    convolve(0)
    pl.semaphore_wait(barrier, 2 * (side_len - 1) + 2 + has_up.astype(jnp.int32) + has_down.astype(jnp.int32))
    for d in range(1, side_len):
        pl.semaphore_signal(ready, inc=1, device_id=in_row(d), device_id_type=MESH)

    send_edges(0)
    for j in blocks[3:]:
        relay(j)
    @pl.when(has_up)
    def _():
        row_up().start()

    @pl.when(has_down)
    def _():
        row_down().start()

    for t in range(3):
        taps = [wv[2 - t, b].astype(F32) for b in range(3)]
        pad = jnp.zeros((OP - outputs, channels), F32)
        tall = jnp.concatenate(
            [taps[0], pad, taps[1], pad, taps[2], pad, jnp.zeros((channels - 3 * OP, channels), F32)], axis=0)
        wb[:, t * channels:(t + 1) * channels] = tall.T.astype(BF)
    pl.semaphore_wait(ready, side_len - 1)
    finish(0)

    @pl.when(has_up)
    def _():
        row_down().wait_recv()

    @pl.when(has_down)
    def _():
        row_up().wait_recv()

    convolve(1)
    send_edges(1)
    convolve(2)
    send_edges(2)
    finish(1)
    finish(2)

    small_copy(1).wait()
    varb[...] = column(var[...], outputs)
    variable = lax.broadcasted_iota(jnp.int32, (OP, LANES), 0)
    for s in range(rounds):
        observed_copy(s).wait()
        buf = stage.at[s % 2]
        buf[0:8 * outputs, :] = obn[s].astype(F32).reshape(8 * outputs, LANES)
        picked = buf[pl.ds(lax.rem(mine[s], 8), OP, stride=8), :]
        obs[s] = jnp.where(variable < outputs, picked, 0.0)

    def col_copy(s, side, dst, k):
        return pltpu.make_async_remote_copy(
            gcol.at[s], dst.at[s], csend.at[s, k], crecv.at[s, k],
            device_id=(me, lat, side), device_id_type=MESH)

    def grad_copy(s, d, to):
        other = lax.rem(me + d, members) if to else lax.rem(me + members - d, members)
        owner = me if to else other
        return pltpu.make_async_remote_copy(
            gout.at[s, other], grad.at[1 + row_at(plan, s, owner)], gsend.at[s, d], grecv.at[s, owner],
            device_id=(other, lat, lon), device_id_type=MESH)

    where = {row: members * s + i for s in range(rounds) for i, row in enumerate(plan[s])}

    def pred_part(s):
        for i in range(members):
            flat_p[pl.ds(i, OP, stride=24), :] = pred[where[members * s + i]].astype(F32)
        pbuf[s] = flat_p[...].reshape(OP, 24, LANES)[:outputs, :members].astype(BF)

    def pred_done(s):
        return pltpu.make_async_copy(pbuf.at[s], pred_out.at[:, pl.ds(members * s, members), :], fsem.at[s])

    def arrive_stage(s):
        def arrive(d, carry):
            pred_copy(s, d, False).wait_recv()
            return carry

        lax.fori_loop(1, members, arrive, 0)
    def pair_stage(s):
        vals = vals_of.at[s]
        vals[...] = block[s].astype(F32)
        row_index = jnp.full((8, LANES), lat * rows + mine[s], jnp.int32).astype(F32)
        angle = -80.0 + 160.0 * (row_index + 0.5) / float(rows * lats)
        lat_weight = jnp.cos(angle * (math.pi / 180.0))

        def slab(k, carry):
            part = pl.ds(pl.multiple_of(8 * k, 8), 8)
            v = vals[:, part, :]
            total = jnp.zeros_like(v)
            for step in range(1, members // 2):
                t = smooth(v - jnp.concatenate([v[step:], v[:step]], axis=0))
                total = total + t - jnp.concatenate([t[members - step:], t[:members - step]], axis=0)
            t = smooth(v[:members // 2] - v[members // 2:])
            total = total + jnp.concatenate([t, -t], axis=0)
            scale = lat_weight * varb[part, :]
            vals[:, part, :] = scale * (smooth(v - obs[s, part, :]) - total / (members - 1))
            return carry

        lax.fori_loop(0, OP // 8, slab, 0)
        collected = jnp.zeros((OP, LANES), F32)
        for j in range(members):
            first = vals[j] if j == 0 else pltpu.roll(vals[j], j, 1)
            collected = jnp.where(lane == j, first, collected)
            collected = jnp.where(lane == 64 + j, pltpu.roll(vals[j], 65 + j, 1), collected)
        gcol[s] = collected.astype(BF)
        col_copy(s, right, gcol_l, 0).start()
        col_copy(s, left, gcol_r, 1).start()

    def return_stage(s):
        vals = vals_of.at[s]
        pred_part(s)
        pred_done(s).start()
        col_copy(s, right, gcol_l, 0).wait_recv()
        col_copy(s, left, gcol_r, 1).wait_recv()
        both = jnp.where(
            lane < 64, pltpu.roll(gcol_l[s].astype(F32), 64, 1), pltpu.roll(gcol_r[s].astype(F32), 64, 1))
        across = jnp.concatenate([both, jnp.zeros((LANES - OP, LANES), F32)], axis=0).T
        for j in range(members):
            vals[j, outputs:outputs + 1, :] = across[j:j + 1]
            vals[j, outputs + 1:outputs + 2, :] = across[64 + j:65 + j]
        gout[s] = vals[...].astype(BF)

        def send(d, carry):
            grad_copy(s, d, True).start()
            return carry

        lax.fori_loop(1, members, send, 0)
        grad[1 + mine[s]] = gout[s, me]

    arrive_stage(0)
    pair_stage(0)
    arrive_stage(1)
    pair_stage(1)
    arrive_stage(2)
    return_stage(0)
    pair_stage(2)
    return_stage(1)
    return_stage(2)

    def return_of(s):
        def arrive_back(d, carry):
            grad_copy(s, d, False).wait_recv()
            return carry

        lax.fori_loop(1, members, arrive_back, 0)

    wb_done = pltpu.make_async_copy(wb, wb_out, fsem.at[rounds + 3])
    wb_done.start()
    return_of(0)
    return_of(1)

    @pl.when(has_up)
    def _():
        grow_up().start()

    @pl.when(has_down)
    def _():
        grow_down().start()

    @pl.when(has_up)
    def _():
        grow_down().wait_recv()

    @pl.when(has_down)
    def _():
        grow_up().wait_recv()

    def slope_copy(k):
        return pltpu.make_async_copy(
            sbuf.at[k], slope_out.at[:, pl.ds(2 * members * k, members), :], fsem.at[rounds + k])

    early = (range(0, members + 1), range(2 * members + 1, rows + 2))
    sides = beyond_columns(grad, [*early[0], *early[1]], outputs, stage.at[0])
    starts = [*range(0, members - 3, 2), members - 3]
    for k, part in enumerate(early):
        for i, g in enumerate(part):
            gs[k, i] = widen(grad, g, sides, g, channels)
        slope_rows(wb, gs.at[k], flat.at[k], starts, k, 24, channels)
        sbuf[k] = flat[k].reshape(channels, 24, LANES)[:, :members].astype(BF)
        slope_copy(k).start()

    return_of(2)
    grad_done = pltpu.make_async_copy(
        grad.at[pl.ds(members - 1, members + 4)], grad_out, fsem.at[rounds + 2])
    grad_done.start()

    for s in range(rounds):
        edge_copy(s, right, edge_l, 0).wait_send()
        edge_copy(s, left, edge_r, 1).wait_send()
        col_copy(s, right, gcol_l, 0).wait_send()
        col_copy(s, left, gcol_r, 1).wait_send()

        def left_device(d, carry):
            pred_copy(s, d, True).wait_send()
            grad_copy(s, d, True).wait_send()
            return carry

        lax.fori_loop(1, members, left_device, 0)

    @pl.when(has_up)
    def _():
        row_up().wait_send()
        grow_up().wait_send()

    @pl.when(has_down)
    def _():
        row_down().wait_send()
        grow_down().wait_send()

    for s in range(rounds):
        pred_done(s).wait()
    for k in range(2):
        slope_copy(k).wait()
    wb_done.wait()
    grad_done.wait()


def backward_kernel(
    members, channels, outputs, grad_in, wb_in, slope_in, pred_in, pred, slope,
    grad, wb, blocks, pbuf, gs, flat, stage, isem, osem,
):
    count = members + 4
    pitch = 2 * members + 8
    ins = [
        pltpu.make_async_copy(grad_in, grad, isem.at[0]),
        pltpu.make_async_copy(wb_in, wb, isem.at[1]),
    ]
    block_at = (0, 1, 4, 5)
    for k, j in enumerate(block_at):
        ins.append(pltpu.make_async_copy(slope_in.at[:, pl.ds(8 * j, 8), :], blocks.at[j], isem.at[2 + k]))
    ins.append(pltpu.make_async_copy(pred_in, pbuf, isem.at[6]))
    for c in ins:
        c.start()

    def out_copy(j):
        return pltpu.make_async_copy(blocks.at[j], slope.at[:, pl.ds(8 * j, 8), :], osem.at[j])

    pred_copy = pltpu.make_async_copy(pbuf, pred, osem.at[6])
    ins[0].wait()
    sides = beyond_columns(grad, range(count), outputs, stage)
    for i in range(count):
        gs[i] = widen(grad, i, sides, i, channels)
    ins[1].wait()
    for k, j in ((2, 0), (5, 5)):
        ins[k].wait()
        out_copy(j).start()
    ins[6].wait()
    pred_copy.start()
    area = (channels, 8, LANES)
    row = lax.broadcasted_iota(jnp.int32, area, 1)

    def computed(j):
        return flat[...].reshape(channels, pitch, LANES)[:, 8 * j - 8:8 * j]

    slope_rows(wb, gs, flat, range(0, 10, 2), 7, pitch, channels)
    blocks[2] = computed(2).astype(BF)
    out_copy(2).start()
    ins[3].wait()
    blocks[1] = jnp.where(row == 7, computed(1), blocks[1].astype(F32)).astype(BF)
    out_copy(1).start()
    slope_rows(wb, gs, flat, range(10, members + 2, 2), 7, pitch, channels)
    blocks[3] = computed(3).astype(BF)
    out_copy(3).start()
    ins[4].wait()
    blocks[4] = jnp.where(row == 0, computed(4), blocks[4].astype(F32)).astype(BF)
    out_copy(4).start()
    for j in range(6):
        out_copy(j).wait()
    pred_copy.wait()


def shards(members, lats, lons, layer_inputs, conv_weight, channel_offset, observed, var_weight):
    channels, rows = layer_inputs.shape[1:3]
    outputs = conv_weight.shape[2]
    rounds = rows // members

    hbm = pl.BlockSpec(memory_space=pltpu.HBM)
    dma = pltpu.SemaphoreType.DMA
    per_member = dma((rounds, members))
    pred_a, grad, wb, slope_a = pl.pallas_call(
        functools.partial(exchange_kernel, members, lats, lons, rounds, channels, outputs),
        out_shape=(
            jax.ShapeDtypeStruct((outputs, rows, LANES), BF),
            jax.ShapeDtypeStruct((members + 4, OP, LANES), BF),
            jax.ShapeDtypeStruct((channels, 3 * channels), BF),
            jax.ShapeDtypeStruct((channels, rows, LANES), BF),
        ),
        in_specs=[hbm] * 5,
        out_specs=(hbm,) * 4,
        scratch_shapes=[
            pltpu.VMEM((rows // 8, channels, 8, LANES), BF),
            pltpu.VMEM((rows + 2, channels, LANES), BF),
            pltpu.VMEM((2, 8 * channels, LANES), F32),
            pltpu.VMEM((3, 3, outputs, channels), BF),
            pltpu.VMEM((3 * OP, 3 * channels), BF),
            pltpu.VMEM((rounds, outputs, 8, LANES), BF),
            pltpu.VMEM((rounds, OP, LANES), F32),
            pltpu.VMEM((1, outputs), F32),
            pltpu.VMEM((1, outputs), F32),
            pltpu.VMEM((OP, LANES), F32),
            pltpu.VMEM((OP, LANES), F32),
            pltpu.VMEM((rows, OP, LANES), F32),
            pltpu.VMEM((rounds, OP, LANES), F32),
            pltpu.VMEM((rounds, OP, LANES), F32),
            pltpu.VMEM((rounds, OP, LANES), F32),
            pltpu.VMEM((rounds, members, OP, LANES), BF),
            pltpu.VMEM((rounds, members, OP, LANES), F32),
            pltpu.VMEM((rounds, members, OP, LANES), BF),
            pltpu.VMEM((rounds, OP, LANES), BF),
            pltpu.VMEM((rounds, OP, LANES), BF),
            pltpu.VMEM((rounds, OP, LANES), BF),
            pltpu.VMEM((rows, OP, LANES), BF),
            pltpu.VMEM((2, members + 2, channels, LANES), BF),
            pltpu.VMEM((2, channels * 24, LANES), F32),
            pltpu.VMEM((OP * 24, LANES), F32),
            pltpu.VMEM((rounds, outputs, members, LANES), BF),
            pltpu.VMEM((2, channels, members, LANES), BF),
            pltpu.VMEM((rows + 2, OP, LANES), BF),
            pltpu.VMEM((channels, 3 * channels), BF),
            dma((rows // 8,)), dma, dma((rounds,)), dma((2,)),
            dma((2,)), dma((2,)), dma((rounds, 2)), dma((rounds, 2)),
            per_member, per_member, per_member, per_member,
            dma((2,)), dma((2,)), dma((rounds, 2)), dma((rounds, 2)), dma((rounds + 4,)), pltpu.SemaphoreType.REGULAR,
        ],
        compiler_params=pltpu.CompilerParams(
            collective_id=0, has_side_effects=True, vmem_limit_bytes=67000000),
        name="exchange",
    )(layer_inputs[0], conv_weight, observed, channel_offset[None], var_weight[None])

    pred, slope = pl.pallas_call(
        functools.partial(backward_kernel, members, channels, outputs),
        out_shape=(
            jax.ShapeDtypeStruct((outputs, rows, LANES), BF),
            jax.ShapeDtypeStruct((channels, rows, LANES), BF),
        ),
        in_specs=[hbm] * 4,
        out_specs=(hbm, hbm),
        scratch_shapes=[
            pltpu.VMEM((members + 4, OP, LANES), BF),
            pltpu.VMEM((channels, 3 * channels), BF),
            pltpu.VMEM((rows // 8, channels, 8, LANES), BF),
            pltpu.VMEM((outputs, rows, LANES), BF),
            pltpu.VMEM((members + 4, channels, LANES), BF),
            pltpu.VMEM((channels * (2 * members + 8), LANES), F32),
            pltpu.VMEM((8 * 64, LANES), F32),
            dma((7,)), dma((7,)),
        ],
        compiler_params=pltpu.CompilerParams(vmem_limit_bytes=67000000),
        name="backward",
    )(grad, wb, slope_a, pred_a)
    return pred[None], slope[None]


def solution(mesh):
    members, lats, lons = (mesh.shape[a] for a in ("member", "lat", "lon"))
    in_specs = (P("member", None, "lat", "lon"), P(), P(), P(None, "lat", "lon"), P())
    out_specs = (P("member", None, "lat", "lon"), P("member", None, "lat", "lon"))
    return jax.shard_map(
        functools.partial(shards, members, lats, lons),
        mesh=mesh, in_specs=in_specs, out_specs=out_specs, check_vma=False)
```

```python
import functools
import math

import jax
import jax.numpy as jnp
from jax import lax
from jax.experimental import pallas as pl
from jax.experimental.pallas import tpu as pltpu
from jax.sharding import PartitionSpec as P

SMOOTHING2 = 0.0625
MESH = pl.DeviceIdType.MESH
BF = jnp.bfloat16
F32 = jnp.float32
OP = 72
LANES = 128


def smooth(d):
    return d * lax.rsqrt(d * d + SMOOTHING2)


def lanes_of(shape):
    return lax.broadcasted_iota(jnp.int32, shape, len(shape) - 1)


def rounds_of(members, rows):
    m = members
    return (
        [*range(1, m - 1), 2 * m + 1, 2 * m + 2],
        [0, m - 1, 2 * m, *range(2 * m + 3, rows)],
        [*range(m, 2 * m)],
    )


def row_at(plan, s, owner):
    listed, members = plan[s], len(plan[s])
    row = owner + listed[0]
    for k in range(1, members):
        jump = listed[k] - listed[k - 1] - 1
        if jump:
            row = row + jump * ((owner + members - k) // members)
    return row


def column(vector, count):
    rows = lax.broadcasted_iota(jnp.int32, (OP, count), 0)
    spread = jnp.where(rows == lanes_of((OP, count)), jnp.broadcast_to(vector, (OP, count)), 0.0)
    return jnp.broadcast_to(jnp.sum(spread, axis=1, keepdims=True), (OP, LANES))


def beyond_columns(grad, indices, outputs, stage):
    last = OP - 8
    for g in indices:
        stage[8 * g:8 * g + 8, :] = grad[g, last:OP, :].astype(F32)
    to_left = stage[pl.ds(outputs - last, 64, stride=8), :]
    to_right = stage[pl.ds(outputs - last + 1, 64, stride=8), :]
    return jnp.concatenate([to_left, to_right], axis=0).T[:OP]


def widen(grad, g, sides, at, channels):
    lane = lanes_of((OP, LANES))
    row = grad[g].astype(F32)
    right = pltpu.roll(sides, (63 - at) % LANES, 1)
    left = sides if at == 0 else pltpu.roll(sides, LANES - at, 1)
    after = jnp.where(lane == LANES - 1, right, pltpu.roll(row, LANES - 1, 1))
    before = jnp.where(lane == 0, left, pltpu.roll(row, 1, 1))
    return jnp.concatenate(
        [after, row, before, jnp.zeros((channels - 3 * OP, LANES), F32)], axis=0).astype(BF)


def slope_rows(wb, gs, flat, starts, shift, pitch, channels):
    for r in starts:
        taps = jnp.concatenate(
            [gs[r:r + 3].reshape(3 * channels, LANES), gs[r + 1:r + 4].reshape(3 * channels, LANES)], axis=1)
        res = jnp.dot(wb[...], taps, preferred_element_type=F32)
        for h in range(2):
            flat[pl.ds(r + h + shift, channels, stride=pitch), :] = res[:, h * LANES:(h + 1) * LANES]


def exchange_kernel(
    members, lats, lons, rounds, channels, outputs,
    xn, weight, observed, offset_in, var_in,
    pred_out, grad_out, wb_out, slope_out,
    xv, xs, stage, wv, wf, obn, obs, offset, var, off, varb, acc, edge, edge_l, edge_r, block, vals_of, gout, gcol, gcol_l, gcol_r, pred, gs, flat, flat_p, pbuf, sbuf, grad, wb,
    xsem, wsem, osem, smem, hsend, hrecv, esend, erecv, psend, precv, gsend, grecv, rsend, rrecv, csend, crecv, fsem, ready,
):
    me = lax.axis_index("member")
    lat = lax.axis_index("lat")
    lon = lax.axis_index("lon")
    left = lax.rem(lon + lons - 1, lons)
    right = lax.rem(lon + 1, lons)
    rows = rounds * members
    has_up = lat > 0
    has_down = lat < lats - 1
    plan = rounds_of(members, rows)
    blocks = (0, 1, 4, 2, 3, 5)
    mine = [row_at(plan, s, me) for s in range(rounds)]

    def block_copy(j):
        return pltpu.make_async_copy(xn.at[:, pl.ds(8 * j, 8), :], xv.at[j], xsem.at[j])

    def weight_copy():
        return pltpu.make_async_copy(weight, wv, wsem)

    def observed_copy(s):
        start = pl.multiple_of(8 * (mine[s] // 8), 8)
        return pltpu.make_async_copy(observed.at[:, pl.ds(start, 8), :], obn.at[s], osem.at[s])

    def small_copy(k):
        return pltpu.make_async_copy((offset_in, var_in)[k], (offset, var)[k], smem.at[k])

    for j in blocks[:2]:
        block_copy(j).start()
    weight_copy().start()
    small_copy(0).start()
    small_copy(1).start()
    for j in blocks[2:]:
        block_copy(j).start()
    for s in range(rounds):
        observed_copy(s).start()

    barrier = pltpu.get_barrier_semaphore()

    side_len = math.isqrt(members)
    own_col, own_row = me // side_len, lax.rem(me, side_len)

    def in_row(d):
        return (own_col * side_len + lax.rem(own_row + d, side_len), lat, lon)

    for d in range(1, side_len):
        pl.semaphore_signal(barrier, inc=1, device_id=in_row(d), device_id_type=MESH)
        pl.semaphore_signal(
            barrier, inc=1, device_id=(lax.rem(me + d * side_len, members), lat, lon), device_id_type=MESH)
    for side in (left, right):
        pl.semaphore_signal(barrier, inc=1, device_id=(me, lat, side), device_id_type=MESH)

    @pl.when(has_up)
    def _():
        pl.semaphore_signal(barrier, inc=1, device_id=(me, lat - 1, lon), device_id_type=MESH)

    @pl.when(has_down)
    def _():
        pl.semaphore_signal(barrier, inc=1, device_id=(me, lat + 1, lon), device_id_type=MESH)

    def row_up():
        return pltpu.make_async_remote_copy(
            xs.at[1], xs.at[rows + 1], hsend.at[0], hrecv.at[0],
            device_id=(me, lat - 1, lon), device_id_type=MESH)

    def row_down():
        return pltpu.make_async_remote_copy(
            xs.at[rows], xs.at[0], hsend.at[1], hrecv.at[1],
            device_id=(me, lat + 1, lon), device_id_type=MESH)

    def grow_up():
        return pltpu.make_async_remote_copy(
            grad.at[1], grad.at[rows + 1], rsend.at[0], rrecv.at[0],
            device_id=(me, lat - 1, lon), device_id_type=MESH)

    def grow_down():
        return pltpu.make_async_remote_copy(
            grad.at[rows], grad.at[0], rsend.at[1], rrecv.at[1],
            device_id=(me, lat + 1, lon), device_id_type=MESH)

    @pl.when(jnp.logical_not(has_up))
    def _():
        xs[0] = jnp.zeros_like(xs[0])
        grad[0] = jnp.zeros_like(grad[0])

    @pl.when(jnp.logical_not(has_down))
    def _():
        xs[rows + 1] = jnp.zeros_like(xs[rows + 1])
        grad[rows + 1] = jnp.zeros_like(grad[rows + 1])

    lane = lanes_of((OP, LANES))

    def edge_copy(s, side, dst, k):
        return pltpu.make_async_remote_copy(
            edge.at[s], dst.at[s], esend.at[s, k], erecv.at[s, k],
            device_id=(me, lat, side), device_id_type=MESH)

    def convolve(s):
        collected = jnp.zeros((OP, LANES), F32)
        for q in range(members // 2):
            taps = jnp.concatenate(
                [xs[r:r + 3].reshape(3 * channels, LANES) for r in plan[s][2 * q:2 * q + 2]], axis=1)
            res = jnp.dot(wf[...], taps, preferred_element_type=F32)
            for h in range(2):
                i = 2 * q + h
                part = res[:, h * LANES:(h + 1) * LANES]
                a0, a1, a2 = part[:OP], part[OP:2 * OP], part[2 * OP:]
                acc[members * s + i] = (
                    a1
                    + jnp.where(lane == 0, 0.0, pltpu.roll(a0, 1, 1))
                    + jnp.where(lane == LANES - 1, 0.0, pltpu.roll(a2, LANES - 1, 1)))
                collected = jnp.where(lane == i, pltpu.roll(a0, 1 + i, 1), collected)
                mine = a2 if i + 64 == 0 else pltpu.roll(a2, 64 + i, 1)
                collected = jnp.where(lane == 64 + i, mine, collected)
        edge[s] = collected

    def send_edges(s):
        edge_copy(s, right, edge_l, 0).start()
        edge_copy(s, left, edge_r, 1).start()

    def pred_copy(s, d, to):
        other = lax.rem(me + d, members) if to else lax.rem(me + members - d, members)
        slot = me if to else other
        return pltpu.make_async_remote_copy(
            pred.at[members * s + other], block.at[s, slot], psend.at[s, d], precv.at[s, slot],
            device_id=(other, lat, lon), device_id_type=MESH)

    def finish(s):
        edge_copy(s, right, edge_l, 0).wait_recv()
        edge_copy(s, left, edge_r, 1).wait_recv()
        for i in range(members):
            from_left = edge_l[s] if i == 0 else pltpu.roll(edge_l[s], LANES - i, 1)
            from_right = pltpu.roll(edge_r[s], 63 - i, 1)
            total = acc[members * s + i] + off[...]
            total = total + jnp.where(lane == 0, from_left, 0.0)
            total = total + jnp.where(lane == LANES - 1, from_right, 0.0)
            pred[members * s + i] = total.astype(BF)

        def send(d, carry):
            pred_copy(s, d, True).start()
            return carry

        lax.fori_loop(1, members, send, 0)
        block[s, me] = pred[members * s + me]

    def relay(j):
        block_copy(j).wait()
        buf = stage.at[j % 2]
        buf[...] = xv[j].astype(F32).reshape(8 * channels, LANES)
        for r in range(8):
            xs[1 + 8 * j + r] = buf[pl.ds(r, channels, stride=8), :].astype(BF)

    weight_copy().wait()
    for a in range(3):
        for b in range(3):
            full = jnp.concatenate(
                [wv[a, b].astype(F32), jnp.zeros((OP - outputs, channels), F32)], axis=0)
            wf[b * OP:(b + 1) * OP, a * channels:(a + 1) * channels] = full.astype(BF)
    small_copy(0).wait()
    off[...] = column(offset[...], outputs)
    for j in blocks[:3]:
        relay(j)
    convolve(0)
    pl.semaphore_wait(barrier, 2 * (side_len - 1) + 2 + has_up.astype(jnp.int32) + has_down.astype(jnp.int32))
    for d in range(1, side_len):
        pl.semaphore_signal(ready, inc=1, device_id=in_row(d), device_id_type=MESH)

    send_edges(0)
    for j in blocks[3:]:
        relay(j)
    @pl.when(has_up)
    def _():
        row_up().start()

    @pl.when(has_down)
    def _():
        row_down().start()

    for t in range(3):
        taps = [wv[2 - t, b].astype(F32) for b in range(3)]
        pad = jnp.zeros((OP - outputs, channels), F32)
        tall = jnp.concatenate(
            [taps[0], pad, taps[1], pad, taps[2], pad, jnp.zeros((channels - 3 * OP, channels), F32)], axis=0)
        wb[:, t * channels:(t + 1) * channels] = tall.T.astype(BF)
    pl.semaphore_wait(ready, side_len - 1)
    finish(0)

    @pl.when(has_up)
    def _():
        row_down().wait_recv()

    @pl.when(has_down)
    def _():
        row_up().wait_recv()

    convolve(1)
    send_edges(1)
    convolve(2)
    send_edges(2)
    finish(1)
    finish(2)

    small_copy(1).wait()
    varb[...] = column(var[...], outputs)
    variable = lax.broadcasted_iota(jnp.int32, (OP, LANES), 0)
    for s in range(rounds):
        observed_copy(s).wait()
        buf = stage.at[s % 2]
        buf[0:8 * outputs, :] = obn[s].astype(F32).reshape(8 * outputs, LANES)
        picked = buf[pl.ds(lax.rem(mine[s], 8), OP, stride=8), :]
        obs[s] = jnp.where(variable < outputs, picked, 0.0)

    def col_copy(s, side, dst, k):
        return pltpu.make_async_remote_copy(
            gcol.at[s], dst.at[s], csend.at[s, k], crecv.at[s, k],
            device_id=(me, lat, side), device_id_type=MESH)

    def grad_copy(s, d, to):
        other = lax.rem(me + d, members) if to else lax.rem(me + members - d, members)
        owner = me if to else other
        return pltpu.make_async_remote_copy(
            gout.at[s, other], grad.at[1 + row_at(plan, s, owner)], gsend.at[s, d], grecv.at[s, owner],
            device_id=(other, lat, lon), device_id_type=MESH)

    where = {row: members * s + i for s in range(rounds) for i, row in enumerate(plan[s])}

    def pred_part(s):
        for i in range(members):
            flat_p[pl.ds(i, OP, stride=24), :] = pred[where[members * s + i]].astype(F32)
        pbuf[s] = flat_p[...].reshape(OP, 24, LANES)[:outputs, :members].astype(BF)

    def pred_done(s):
        return pltpu.make_async_copy(pbuf.at[s], pred_out.at[:, pl.ds(members * s, members), :], fsem.at[s])

    def arrive_stage(s):
        def arrive(d, carry):
            pred_copy(s, d, False).wait_recv()
            return carry

        lax.fori_loop(1, members, arrive, 0)
    def pair_stage(s):
        vals = vals_of.at[s]
        vals[...] = block[s].astype(F32)
        row_index = jnp.full((8, LANES), lat * rows + mine[s], jnp.int32).astype(F32)
        angle = -80.0 + 160.0 * (row_index + 0.5) / float(rows * lats)
        lat_weight = jnp.cos(angle * (math.pi / 180.0))

        def slab(k, carry):
            part = pl.ds(pl.multiple_of(8 * k, 8), 8)
            v = vals[:, part, :]
            total = jnp.zeros_like(v)
            for step in range(1, members // 2):
                t = smooth(v - jnp.concatenate([v[step:], v[:step]], axis=0))
                total = total + t - jnp.concatenate([t[members - step:], t[:members - step]], axis=0)
            t = smooth(v[:members // 2] - v[members // 2:])
            total = total + jnp.concatenate([t, -t], axis=0)
            scale = lat_weight * varb[part, :]
            vals[:, part, :] = scale * (smooth(v - obs[s, part, :]) - total / (members - 1))
            return carry

        lax.fori_loop(0, OP // 8, slab, 0, unroll=3)
        collected = jnp.zeros((OP, LANES), F32)
        for j in range(members):
            first = vals[j] if j == 0 else pltpu.roll(vals[j], j, 1)
            collected = jnp.where(lane == j, first, collected)
            collected = jnp.where(lane == 64 + j, pltpu.roll(vals[j], 65 + j, 1), collected)
        gcol[s] = collected.astype(BF)
        col_copy(s, right, gcol_l, 0).start()
        col_copy(s, left, gcol_r, 1).start()

    def return_stage(s):
        vals = vals_of.at[s]
        pred_part(s)
        pred_done(s).start()
        col_copy(s, right, gcol_l, 0).wait_recv()
        col_copy(s, left, gcol_r, 1).wait_recv()
        both = jnp.where(
            lane < 64, pltpu.roll(gcol_l[s].astype(F32), 64, 1), pltpu.roll(gcol_r[s].astype(F32), 64, 1))
        across = jnp.concatenate([both, jnp.zeros((LANES - OP, LANES), F32)], axis=0).T
        for j in range(members):
            vals[j, outputs:outputs + 1, :] = across[j:j + 1]
            vals[j, outputs + 1:outputs + 2, :] = across[64 + j:65 + j]
        gout[s] = vals[...].astype(BF)

        def send(d, carry):
            grad_copy(s, d, True).start()
            return carry

        lax.fori_loop(1, members, send, 0)
        grad[1 + mine[s]] = gout[s, me]

    arrive_stage(0)
    pair_stage(0)
    arrive_stage(1)
    pair_stage(1)
    arrive_stage(2)
    return_stage(0)
    pair_stage(2)
    return_stage(1)
    return_stage(2)

    def return_of(s):
        def arrive_back(d, carry):
            grad_copy(s, d, False).wait_recv()
            return carry

        lax.fori_loop(1, members, arrive_back, 0)

    wb_done = pltpu.make_async_copy(wb, wb_out, fsem.at[rounds + 3])
    wb_done.start()
    return_of(0)
    return_of(1)

    @pl.when(has_up)
    def _():
        grow_up().start()

    @pl.when(has_down)
    def _():
        grow_down().start()

    @pl.when(has_up)
    def _():
        grow_down().wait_recv()

    @pl.when(has_down)
    def _():
        grow_up().wait_recv()

    def slope_copy(k):
        return pltpu.make_async_copy(
            sbuf.at[k], slope_out.at[:, pl.ds(2 * members * k, members), :], fsem.at[rounds + k])

    early = (range(0, members + 1), range(2 * members + 1, rows + 2))
    sides = beyond_columns(grad, [*early[0], *early[1]], outputs, stage.at[0])
    starts = [*range(0, members - 3, 2), members - 3]
    for k, part in enumerate(early):
        for i, g in enumerate(part):
            gs[k, i] = widen(grad, g, sides, g, channels)
        slope_rows(wb, gs.at[k], flat.at[k], starts, k, 24, channels)
        sbuf[k] = flat[k].reshape(channels, 24, LANES)[:, :members].astype(BF)
        slope_copy(k).start()

    return_of(2)
    grad_done = pltpu.make_async_copy(
        grad.at[pl.ds(members - 1, members + 4)], grad_out, fsem.at[rounds + 2])
    grad_done.start()

    for s in range(rounds):
        edge_copy(s, right, edge_l, 0).wait_send()
        edge_copy(s, left, edge_r, 1).wait_send()
        col_copy(s, right, gcol_l, 0).wait_send()
        col_copy(s, left, gcol_r, 1).wait_send()

        def left_device(d, carry):
            pred_copy(s, d, True).wait_send()
            grad_copy(s, d, True).wait_send()
            return carry

        lax.fori_loop(1, members, left_device, 0)

    @pl.when(has_up)
    def _():
        row_up().wait_send()
        grow_up().wait_send()

    @pl.when(has_down)
    def _():
        row_down().wait_send()
        grow_down().wait_send()

    for s in range(rounds):
        pred_done(s).wait()
    for k in range(2):
        slope_copy(k).wait()
    wb_done.wait()
    grad_done.wait()


def backward_kernel(
    members, channels, outputs, grad_in, wb_in, slope_in, pred_in, pred, slope,
    grad, wb, blocks, pbuf, gs, flat, stage, isem, osem,
):
    count = members + 4
    pitch = 2 * members + 8
    ins = [
        pltpu.make_async_copy(grad_in, grad, isem.at[0]),
        pltpu.make_async_copy(wb_in, wb, isem.at[1]),
    ]
    block_at = (0, 1, 4, 5)
    for k, j in enumerate(block_at):
        ins.append(pltpu.make_async_copy(slope_in.at[:, pl.ds(8 * j, 8), :], blocks.at[j], isem.at[2 + k]))
    ins.append(pltpu.make_async_copy(pred_in, pbuf, isem.at[6]))
    for c in ins:
        c.start()

    def out_copy(j):
        return pltpu.make_async_copy(blocks.at[j], slope.at[:, pl.ds(8 * j, 8), :], osem.at[j])

    pred_copy = pltpu.make_async_copy(pbuf, pred, osem.at[6])
    ins[0].wait()
    sides = beyond_columns(grad, range(count), outputs, stage)
    for i in range(count):
        gs[i] = widen(grad, i, sides, i, channels)
    ins[1].wait()
    for k, j in ((2, 0), (5, 5)):
        ins[k].wait()
        out_copy(j).start()
    ins[6].wait()
    pred_copy.start()
    area = (channels, 8, LANES)
    row = lax.broadcasted_iota(jnp.int32, area, 1)

    def computed(j):
        return flat[...].reshape(channels, pitch, LANES)[:, 8 * j - 8:8 * j]

    slope_rows(wb, gs, flat, range(0, 10, 2), 7, pitch, channels)
    blocks[2] = computed(2).astype(BF)
    out_copy(2).start()
    ins[3].wait()
    blocks[1] = jnp.where(row == 7, computed(1), blocks[1].astype(F32)).astype(BF)
    out_copy(1).start()
    slope_rows(wb, gs, flat, range(10, members + 2, 2), 7, pitch, channels)
    blocks[3] = computed(3).astype(BF)
    out_copy(3).start()
    ins[4].wait()
    blocks[4] = jnp.where(row == 0, computed(4), blocks[4].astype(F32)).astype(BF)
    out_copy(4).start()
    for j in range(6):
        out_copy(j).wait()
    pred_copy.wait()


def shards(members, lats, lons, layer_inputs, conv_weight, channel_offset, observed, var_weight):
    channels, rows = layer_inputs.shape[1:3]
    outputs = conv_weight.shape[2]
    rounds = rows // members

    hbm = pl.BlockSpec(memory_space=pltpu.HBM)
    dma = pltpu.SemaphoreType.DMA
    per_member = dma((rounds, members))
    pred_a, grad, wb, slope_a = pl.pallas_call(
        functools.partial(exchange_kernel, members, lats, lons, rounds, channels, outputs),
        out_shape=(
            jax.ShapeDtypeStruct((outputs, rows, LANES), BF),
            jax.ShapeDtypeStruct((members + 4, OP, LANES), BF),
            jax.ShapeDtypeStruct((channels, 3 * channels), BF),
            jax.ShapeDtypeStruct((channels, rows, LANES), BF),
        ),
        in_specs=[hbm] * 5,
        out_specs=(hbm,) * 4,
        scratch_shapes=[
            pltpu.VMEM((rows // 8, channels, 8, LANES), BF),
            pltpu.VMEM((rows + 2, channels, LANES), BF),
            pltpu.VMEM((2, 8 * channels, LANES), F32),
            pltpu.VMEM((3, 3, outputs, channels), BF),
            pltpu.VMEM((3 * OP, 3 * channels), BF),
            pltpu.VMEM((rounds, outputs, 8, LANES), BF),
            pltpu.VMEM((rounds, OP, LANES), F32),
            pltpu.VMEM((1, outputs), F32),
            pltpu.VMEM((1, outputs), F32),
            pltpu.VMEM((OP, LANES), F32),
            pltpu.VMEM((OP, LANES), F32),
            pltpu.VMEM((rows, OP, LANES), F32),
            pltpu.VMEM((rounds, OP, LANES), F32),
            pltpu.VMEM((rounds, OP, LANES), F32),
            pltpu.VMEM((rounds, OP, LANES), F32),
            pltpu.VMEM((rounds, members, OP, LANES), BF),
            pltpu.VMEM((rounds, members, OP, LANES), F32),
            pltpu.VMEM((rounds, members, OP, LANES), BF),
            pltpu.VMEM((rounds, OP, LANES), BF),
            pltpu.VMEM((rounds, OP, LANES), BF),
            pltpu.VMEM((rounds, OP, LANES), BF),
            pltpu.VMEM((rows, OP, LANES), BF),
            pltpu.VMEM((2, members + 2, channels, LANES), BF),
            pltpu.VMEM((2, channels * 24, LANES), F32),
            pltpu.VMEM((OP * 24, LANES), F32),
            pltpu.VMEM((rounds, outputs, members, LANES), BF),
            pltpu.VMEM((2, channels, members, LANES), BF),
            pltpu.VMEM((rows + 2, OP, LANES), BF),
            pltpu.VMEM((channels, 3 * channels), BF),
            dma((rows // 8,)), dma, dma((rounds,)), dma((2,)),
            dma((2,)), dma((2,)), dma((rounds, 2)), dma((rounds, 2)),
            per_member, per_member, per_member, per_member,
            dma((2,)), dma((2,)), dma((rounds, 2)), dma((rounds, 2)), dma((rounds + 4,)), pltpu.SemaphoreType.REGULAR,
        ],
        compiler_params=pltpu.CompilerParams(
            collective_id=0, has_side_effects=True, vmem_limit_bytes=67000000),
        name="exchange",
    )(layer_inputs[0], conv_weight, observed, channel_offset[None], var_weight[None])

    pred, slope = pl.pallas_call(
        functools.partial(backward_kernel, members, channels, outputs),
        out_shape=(
            jax.ShapeDtypeStruct((outputs, rows, LANES), BF),
            jax.ShapeDtypeStruct((channels, rows, LANES), BF),
        ),
        in_specs=[hbm] * 4,
        out_specs=(hbm, hbm),
        scratch_shapes=[
            pltpu.VMEM((members + 4, OP, LANES), BF),
            pltpu.VMEM((channels, 3 * channels), BF),
            pltpu.VMEM((rows // 8, channels, 8, LANES), BF),
            pltpu.VMEM((outputs, rows, LANES), BF),
            pltpu.VMEM((members + 4, channels, LANES), BF),
            pltpu.VMEM((channels * (2 * members + 8), LANES), F32),
            pltpu.VMEM((8 * 64, LANES), F32),
            dma((7,)), dma((7,)),
        ],
        compiler_params=pltpu.CompilerParams(vmem_limit_bytes=67000000),
        name="backward",
    )(grad, wb, slope_a, pred_a)
    return pred[None], slope[None]


def solution(mesh):
    members, lats, lons = (mesh.shape[a] for a in ("member", "lat", "lon"))
    in_specs = (P("member", None, "lat", "lon"), P(), P(), P(None, "lat", "lon"), P())
    out_specs = (P("member", None, "lat", "lon"), P("member", None, "lat", "lon"))
    return jax.shard_map(
        functools.partial(shards, members, lats, lons),
        mesh=mesh, in_specs=in_specs, out_specs=out_specs, check_vma=False)
```
